32 devices in a mesh: fsdp: 8 (over y, x, core), tp: 4 (over z).
Axes of the slice: x: 2, y: 2, z: 4, core: 2. Of those that a mesh axis runs over, the one named last changes fastest.
Arguments:
- partials: bfloat16 [8, 2, 5120, 1024], P('fsdp', None, None, 'tp'), may hold values from -6 to 6
- token_counts: int32 [8], P('fsdp'), may hold values from 100 to 599
- owner_map: int32 [2, 4], replicated, may hold values from 0 to 3, each once within a row
- params: float32 [2, 5120, 1024], P(None, 'fsdp', 'tp'), may hold values from -0.75 to 0.75
- moment1: float32 [2, 5120, 1024], P(None, 'fsdp', 'tp'), may hold values from -0.15625 to 0.15625
- moment2: float32 [2, 5120, 1024], P(None, 'fsdp', 'tp'), may hold values from 0.0001 to 0.004
Outputs:
- new_params: float32 [2, 5120, 1024], P(None, 'fsdp', 'tp')
- new_moment1: float32 [2, 5120, 1024], P(None, 'fsdp', 'tp')
- new_moment2: float32 [2, 5120, 1024], P(None, 'fsdp', 'tp')
- rollout_delta: bfloat16 [2, 5120, 1024], P(None, None, 'tp')
The draws below stay inside these ranges and needn't reach their ends.
Inputs may be any that keep to these rules, and one draw needn't show every extreme that they name: `owner_map`: each row is a permutation of 0 to 3.
All inputs are finite; a program needn't handle non-finite values.
Results may differ from the reference program's by a relative error of at most 0.0004.
Values may be sent and summed in bfloat16 or wider, within the bound.
A program may use at most 64 MiB of HBM per device.

```python
import math
import jax
import jax.numpy as jnp
from jax import lax

D = 5120
KV = 1024
LAYERS = 2
STEP = 10
N_FSDP = 8
N_TP = 4


def draw_token_counts(key, part):
    base = jax.random.randint(key, (N_FSDP,), 100, 200)
    ramp = jnp.arange(N_FSDP, dtype=jnp.int32) * 400 // max(N_FSDP - 1, 1)
    position = jnp.arange(N_FSDP, dtype=jnp.int32)
    counts = jnp.where(position == 0, 100, base + ramp)
    counts = jnp.where(position == N_FSDP - 1, 599, counts)
    return counts.astype(jnp.int32)


def spiked(values, own_key, source, target, shards_of, factor):
    def block_of(dim):
        return (jnp.arange(values.shape[dim]) // (values.shape[dim] // shards_of)).reshape((-1,) + (1,) * (values.ndim - 1 - dim))

    near = jax.random.permutation(own_key, shards_of)[block_of(target)]
    far = (block_of(target) + shards_of // 2) % shards_of
    return jnp.where((block_of(source) == near) | (block_of(source) == far), factor * values, values)


def block_levels(key, shape, cuts, least, largest):
    loudness = 1.0
    for dim, blocks in cuts:
        draws = jax.random.uniform(jax.random.fold_in(jax.random.fold_in(key, 6), dim), (blocks,), jnp.float32, least / len(cuts), largest / len(cuts))
        loudness = loudness * jnp.repeat(jnp.exp(draws), shape[dim] // blocks).reshape((-1,) + (1,) * (len(shape) - 1 - dim))
    return loudness


def scatter_about(stream_key, dims, width, limit, pieces=(), held_as=jnp.bfloat16):
    drawn = jax.random.normal(stream_key, dims, jnp.float32) * width
    if len(pieces) > 0:
        drawn = block_levels(stream_key, dims, pieces, -0.22, 0.18) * drawn
    return jnp.clip(drawn, min=-limit, max=limit).astype(held_as)


def bell_draw_with(rng, extent, scale, reach, split, heavy, kind=jnp.bfloat16):
    drawn = scale * jax.random.normal(rng, extent, jnp.float32)
    if split:
        drawn = drawn * block_levels(rng, extent, split, -0.22, 0.18)
    return jnp.clip(spiked(drawn, jax.random.fold_in(rng, 3), *heavy), -reach, reach).astype(kind)


def setup_inputs(seed: int = 0) -> dict:
    streams_of = jax.random.split(jax.random.key(seed), 7)
    return {
        "partials": bell_draw_with(streams_of[0], (N_FSDP, LAYERS, D, KV), 1.0, 6.0, ((0, 8), (3, 4)), (0, 2, 8, 2.0)),
        "token_counts": draw_token_counts(jax.random.fold_in(streams_of[6], 71), 0),
        "owner_map": jax.vmap(lambda own: jax.random.permutation(own, N_TP))(jax.random.split(streams_of[2], LAYERS)).reshape((LAYERS, N_TP)).astype(jnp.int32),
        "params": scatter_about(streams_of[3], (LAYERS, D, KV), 0.05, 0.75, ((1, 8), (2, 4)), jnp.float32),
        "moment1": scatter_about(streams_of[4], (LAYERS, D, KV), 0.01, 0.15625, ((1, 8), (2, 4)), jnp.float32),
        "moment2": jnp.clip(jnp.exp(math.log(0.004) - 3.6888795 * jax.random.uniform(streams_of[5], (LAYERS, D, KV), jnp.float32) ** block_levels(streams_of[5], (LAYERS, D, KV), ((1, 8), (2, 4)), -0.2, 0.2)), 0.0001, 0.004),
    }


def reference(partials, token_counts, owner_map, params, moment1, moment2):
    weights = token_counts.astype(jnp.float32)
    total = jnp.sum(weights)

    def accumulate(summed, pair):
        term, weight = pair
        return (summed + weight * term.astype(jnp.float32), None)
    summed, _ = lax.scan(accumulate, jnp.zeros((LAYERS, D, KV), jnp.float32), (partials, weights))
    grad = summed / total
    first = 0.9 * moment1 + 0.1 * grad
    second = 0.999 * moment2 + 0.001 * grad * grad
    bias_one = 1.0 - 0.9 ** STEP
    bias_two = 1.0 - 0.999 ** STEP
    direction = first / bias_one / (jnp.sqrt(second / bias_two) + 1e-08)
    new_params = params - 0.001 * (direction + 0.1 * params)
    delta = direction.astype(jnp.bfloat16)
    blocks = delta.reshape(LAYERS, D, N_TP, KV // N_TP)
    chosen = owner_map.astype(jnp.int32)[:, None, :, None]
    rollout = jnp.take_along_axis(blocks, chosen, axis=2).reshape(LAYERS, D, KV)
    return (new_params, first, second, rollout)
```

```python
import functools

import jax
import jax.numpy as jnp
from jax import lax
from jax.experimental import pallas as pl
from jax.experimental.pallas import tpu as pltpu
from jax.sharding import PartitionSpec as P

STEP = 10
MESH = pl.DeviceIdType.MESH
SPLIT = 8
TILE = 16
SPAN = 80
AHEAD = 2
LATE = 3


def plain(partials, token_counts, owner_map, params, moment1, moment2):
    weight = token_counts.astype(jnp.float32)[0]
    total = lax.psum(weight, "fsdp")
    summed = lax.psum_scatter(
        weight * partials[0].astype(jnp.float32), "fsdp", scatter_dimension=1, tiled=True
    )
    first, second, direction, new_params = adam(summed * (1.0 / total), params, moment1, moment2)
    delta = direction.astype(jnp.bfloat16)
    owners = lax.axis_size("tp")
    served = lax.dynamic_index_in_dim(owner_map, lax.axis_index("tp"), 1, keepdims=False)
    blocks = lax.all_gather(delta, "tp", axis=0)
    kept = jnp.take_along_axis(blocks, served[None, :, None, None], axis=0)[0]
    rollout = lax.all_gather(kept, "fsdp", axis=1, tiled=True)
    return (new_params, first, second, rollout)


def adam(grad, params, moment1, moment2):
    first = 0.9 * moment1 + 0.1 * grad
    second = 0.999 * moment2 + 0.001 * grad * grad
    scale_one = 1.0 / (1.0 - 0.9**STEP)
    scale_two = 1.0 / (1.0 - 0.999**STEP)
    direction = first * scale_one / (jnp.sqrt(second * scale_two) + 1e-08)
    new_params = params - 0.001 * (direction + 0.1 * params)
    return first, second, direction, new_params


def kernel(
    sizes,
    owner_ref,
    count_ref,
    part_ref,
    p_ref,
    m_ref,
    v_ref,
    np_ref,
    nm_ref,
    nv_ref,
    roll_ref,
    own_w,
    wbuf,
    mine,
    theirs,
    near,
    acc,
    recv,
    held,
    cross,
    w_s,
    w_r,
    opt_s,
    ld_s,
    raw_s,
    raw_r,
    near_s,
    near_r,
    rs_s,
    rs_r,
    z_s,
    z_r,
    ag_s,
    ag_r,
    fin_s,
    fin_r,
):
    layers, fsdp, tp, parts, rows = sizes
    chunks = layers * parts
    pairs = fsdp // 2
    kept = pairs // 2
    bits = pairs.bit_length() - 1
    me = lax.axis_index("fsdp")
    col = lax.axis_index("tp")
    core = lax.rem(me, 2)
    mine_q = me // 2
    partner = mine_q * 2 + (1 - core)

    def away(index, flips):
        q = index
        for b in flips:
            q = q + (1 - 2 * lax.rem(index // (1 << b), 2)) * (1 << b)
        return q

    def ones(number):
        return [b for b in range(number.bit_length()) if number >> b & 1]

    tp_bits = tp.bit_length() - 1
    barrier = pltpu.get_barrier_semaphore()
    for d in range(1, fsdp):
        pl.semaphore_signal(
            barrier, inc=1, device_id={"fsdp": lax.rem(me + d, fsdp)}, device_id_type=MESH
        )
    for b in range(tp_bits):
        pl.semaphore_signal(
            barrier, inc=1, device_id={"tp": away(col, [b])}, device_id_type=MESH
        )

    def where(c):
        return c // parts, c % parts

    def order(c):
        names = list(range(bits))
        return names if c % 2 == 0 else names[::-1]

    def flipped(flips):
        return away(mine_q, flips)

    def block_of(c, pos):
        return flipped([order(c)[i] for i in range(bits) if pos >> (bits - 1 - i) & 1])

    own_w[...] = jnp.full(own_w.shape, count_ref[0], jnp.int32).astype(jnp.float32)
    for c in range(chunks):
        l, k = where(c)
        for pos in range(kept):
            pltpu.make_async_copy(
                part_ref.at[l, block_of(c, pos), core, k], mine.at[c, pos], ld_s.at[c]
            ).start()
    pl.semaphore_wait(barrier, fsdp - 1 + tp_bits)

    def push(src, dst, send, arrive, **device):
        copy = pltpu.make_async_remote_copy(
            src_ref=src,
            dst_ref=dst,
            send_sem=send,
            recv_sem=arrive,
            device_id=device,
            device_id_type=MESH,
        )
        copy.start()
        return copy

    weights = []
    for d in range(1, fsdp):
        weights.append(
            push(own_w, wbuf.at[d], w_s.at[d], w_r.at[d], fsdp=lax.rem(me + d, fsdp))
        )

    def pass_on(c):
        l, k = where(c)
        there = flipped([order(c)[0]])
        for pos in range(kept):
            for half in range(2):
                push(
                    part_ref.at[l, block_of(c, kept + pos), half, k],
                    near.at[c, core, pos],
                    near_s.at[c],
                    near_r.at[c],
                    fsdp=there * 2 + half,
                )

    def share(c):
        l, k = where(c)
        for pos in range(kept):
            push(
                part_ref.at[l, block_of(c, pos), 1 - core, k],
                theirs.at[c, pos],
                raw_s.at[c],
                raw_r.at[c],
                fsdp=partner,
            )

    groups = [tuple(range(c, min(c + 2, chunks))) for c in range(0, chunks, 2)]
    for group in groups[:AHEAD]:
        for c in group:
            share(c)
            pass_on(c)
    for group in groups[AHEAD:]:
        for c in group:
            share(c)
    opts = []
    for i, (src, dst) in enumerate(((p_ref, np_ref), (m_ref, nm_ref), (v_ref, nv_ref))):
        load = pltpu.make_async_copy(src, dst, opt_s.at[i])
        load.start()
        opts.append(load)

    lanes = own_w.shape[1]
    width = mine.shape[3]

    def row(tile):
        return jnp.concatenate([tile[0:1, :]] * (width // lanes), axis=1)

    my_weight = row(own_w[...])
    met_weights = []

    def weight_of(index):
        return row(wbuf[lax.rem(me - index + fsdp, fsdp)])

    def weigh():
        total = my_weight
        for d in range(1, fsdp):
            weights[d - 1].wait()
            total = total + row(wbuf[d])
        met_weights.append(1.0 / total)
        met_weights.append(weight_of(partner))
        for b in range(bits):
            met_weights.append([weight_of(flipped([b]) * 2 + half) for half in range(2)])

    step = next(n for n in range(min(rows, SPAN), 0, -TILE) if rows % n == 0)

    def tiles(body):
        def run(i, carry):
            body(pl.ds(pl.multiple_of(i * step, step), step))
            return carry

        lax.fori_loop(0, rows // step, run, 0)

    halving = {}
    spread = {}

    def halve(c, i):
        half = pairs >> (i + 1)
        there = flipped([order(c)[i]]) * 2 + core
        halving[c, i] = push(
            acc.at[c, pl.ds(half, half)],
            recv.at[c, pl.ds(half, half)],
            rs_s.at[c, i],
            rs_r.at[c, i],
            fsdp=there,
        )

    def held_rows(c, pos):
        q = flipped([order(c)[b] for b in ones(pos)])
        l, k = where(c)
        return roll_ref.at[l, q, core, k]

    def double(c, j):
        there = flipped([order(c)[j]]) * 2 + core
        for pos in range(1 << j):
            block = held_rows(c, pos)
            push(block, block, ag_s.at[c, j], ag_r.at[c, j], fsdp=there)

    def await_part(part, sem):
        pltpu.make_async_copy(part, part, sem).wait()

    def await_blocks(c, count, sem):
        l, k = where(c)
        await_part(near.at[c, 0, pl.ds(0, count)], sem)

    def gather_sum(c):
        await_part(mine.at[c], ld_s.at[c])
        await_part(theirs.at[c], raw_r.at[c])
        await_part(near.at[c], near_r.at[c])
        if c == 0:
            weigh()
        other_weight = met_weights[1]
        near_weights = met_weights[2 + order(c)[0]]
        for pos in range(kept - 1, -1, -1):

            def body(at):
                total = my_weight * mine[c, pos, at, :].astype(jnp.float32)
                total = total + other_weight * theirs[c, pos, at, :].astype(jnp.float32)
                for half in range(2):
                    total = total + near_weights[half] * near[c, half, pos, at, :].astype(
                        jnp.float32
                    )
                acc[c, pos, at, :] = total

            tiles(body)
            if bits > 1 and pos == kept // 2:
                halve(c, 1)

    def add(i, c):
        halving[c, i].wait_recv()
        half = pairs >> (i + 1)
        for pos in range(half - 1, -1, -1):

            def body(at):
                acc[c, pos, at, :] = acc[c, pos, at, :] + recv[c, half + pos, at, :]

            tiles(body)
            if pos == half // 2:
                halve(c, i + 1)

    def update(c):
        l, k = where(c)
        if bits > 1:
            halving[c, bits - 1].wait_recv()
        if c == 0:
            for load in opts:
                load.wait()
        scale = met_weights[0]

        def body(at):
            total = acc[c, 0, at, :]
            if bits > 1:
                total = total + recv[c, 1, at, :]
            first, second, direction, new_params = adam(
                total * scale, np_ref[l, k, at, :], nm_ref[l, k, at, :], nv_ref[l, k, at, :]
            )
            held[c, 0, at, :] = direction.astype(jnp.bfloat16)
            np_ref[l, k, at, :] = new_params
            nm_ref[l, k, at, :] = first
            nv_ref[l, k, at, :] = second

        tiles(body)
        if tp_bits > 1:
            meet(c, 0)
        else:
            hand_over(c)

    def meet(c, b):
        size = 1 << b
        spread[c, b] = push(
            held.at[c, pl.ds(0, size)],
            held.at[c, pl.ds(size, size)],
            z_s.at[c, b],
            z_r.at[c, b],
            tp=away(col, [b]),
        )

    def pick(c, at, served, start):
        chosen = start
        for slot in range(tp // 2):
            chosen = jnp.where(
                served == away(col, ones(slot)), held[c, slot, at, :].astype(jnp.float32), chosen
            )
        return chosen.astype(jnp.bfloat16)

    def hand_over(c):
        l, k = where(c)
        there = away(col, [tp_bits - 1])
        served = owner_ref[l, there]

        def body(at):
            cross[c, 0, at, :] = pick(c, at, served, held[c, 0, at, :].astype(jnp.float32))

        tiles(body)
        spread[c, tp_bits - 1] = push(
            cross.at[c, 0],
            cross.at[c, 1],
            z_s.at[c, tp_bits - 1],
            z_r.at[c, tp_bits - 1],
            tp=there,
        )

    def met(b, c):
        spread[c, b].wait_recv()
        if b + 2 < tp_bits:
            meet(c, b + 1)
        else:
            hand_over(c)

    def select(c):
        l, k = where(c)
        spread[c, tp_bits - 1].wait_recv()
        served = owner_ref[l, col]

        def body(at):
            roll_ref[l, mine_q, core, k, at, :] = pick(
                c, at, served, cross[c, 1, at, :].astype(jnp.float32)
            )

        tiles(body)
        double(c, 0)
        finish(c, 0, 1)

    def finish(c, first, count):
        for pos in range(first, first + count):
            block = held_rows(c, pos)
            push(block, block, fin_s.at[c], fin_r.at[c], fsdp=partner)

    def forward(j, c):
        await_blocks(c, 1 << j, ag_r.at[c, j])
        if j + 1 < bits:
            double(c, j + 1)
        finish(c, 1 << j, 1 << j)

    stages = [gather_sum]
    stages += [functools.partial(add, i) for i in range(1, bits - 1)]
    stages += [update]
    stages += [functools.partial(met, b) for b in range(tp_bits - 1)]
    lags = list(range(len(stages)))
    tail = [select] + [functools.partial(forward, j) for j in range(bits)]
    lags += [len(stages) + LATE + i for i in range(len(tail))]
    stages += tail
    for t in range(len(groups) + lags[-1]):
        for lag, stage in zip(lags, stages):
            if 0 <= t - lag < len(groups):
                for c in groups[t - lag]:
                    stage(c)
            if lag == 0 and t + AHEAD < len(groups):
                for c in groups[t + AHEAD]:
                    pass_on(c)

    for c in range(chunks):
        await_part(theirs.at[c], raw_s.at[c])
        await_part(near.at[c], near_s.at[c])
        for i in range(1, bits):
            halving[c, i].wait_send()
        for i in range(bits):
            await_blocks(c, 1 << i, ag_s.at[c, i])
        for b in range(tp_bits):
            spread[c, b].wait_send()
        for sem in (fin_s, fin_r):
            await_part(roll_ref.at[0, :, 0, 0], sem.at[c])


def write_out(*refs):
    count = len(refs) // 2
    copies = []
    for i in range(count):
        for l in range(refs[i].shape[0]):
            sem = refs[-1].at[i, l]
            copies.append(pltpu.make_async_copy(refs[i].at[l], refs[count + i].at[l], sem))
    for copy in copies:
        copy.start()
    for copy in copies:
        copy.wait()


def fused(fsdp, tp, partials, token_counts, owner_map, params, moment1, moment2):
    layers, depth, width = partials.shape[1:]
    per = params.shape[1]
    pairs = fsdp // 2
    bits = pairs.bit_length() - 1
    tp_bits = tp.bit_length() - 1
    parts = next(n for n in range(SPLIT, 0, -1) if per % (n * TILE) == 0)
    rows = per // parts
    chunks = layers * parts
    lanes = 128 if width % 128 == 0 else width
    anywhere = pl.BlockSpec(memory_space=pl.ANY)
    dma = pltpu.SemaphoreType.DMA
    state = (layers, parts, rows, width)
    f32, b16 = jnp.float32, jnp.bfloat16
    outs = pl.pallas_call(
        functools.partial(kernel, (layers, fsdp, tp, parts, rows)),
        out_shape=[
            pltpu.VMEM(state, f32),
            pltpu.VMEM(state, f32),
            pltpu.VMEM(state, f32),
            pltpu.VMEM((layers, pairs, 2, parts, rows, width), b16),
        ],
        in_specs=[
            pl.BlockSpec(memory_space=pltpu.SMEM),
            pl.BlockSpec(memory_space=pltpu.SMEM),
            anywhere,
            anywhere,
            anywhere,
            anywhere,
        ],
        out_specs=[pl.BlockSpec(memory_space=pltpu.VMEM)] * 4,
        scratch_shapes=[
            pltpu.VMEM((8, lanes), f32),
            pltpu.VMEM((fsdp, 8, lanes), f32),
            pltpu.VMEM((chunks, pairs // 2, rows, width), b16),
            pltpu.VMEM((chunks, pairs // 2, rows, width), b16),
            pltpu.VMEM((chunks, 2, pairs // 2, rows, width), b16),
            pltpu.VMEM((chunks, pairs // 2, rows, width), f32),
            pltpu.VMEM((chunks, pairs // 2, rows, width), f32),
            pltpu.VMEM((chunks, tp // 2, rows, width), b16),
            pltpu.VMEM((chunks, 2, rows, width), b16),
            dma((fsdp,)),
            dma((fsdp,)),
            dma((3,)),
            dma((chunks,)),
            dma((chunks,)),
            dma((chunks,)),
            dma((chunks,)),
            dma((chunks,)),
            dma((chunks, bits)),
            dma((chunks, bits)),
            dma((chunks, tp_bits)),
            dma((chunks, tp_bits)),
            dma((chunks, bits)),
            dma((chunks, bits)),
            dma((chunks,)),
            dma((chunks,)),
        ],
        compiler_params=pltpu.CompilerParams(
            collective_id=0, has_side_effects=True, vmem_limit_bytes=48 * 1024 * 1024
        ),
    )(
        owner_map,
        token_counts,
        partials.reshape(layers, pairs, 2, parts, rows, width),
        params.reshape(state),
        moment1.reshape(state),
        moment2.reshape(state),
    )
    outs = [out.reshape(params.shape) for out in outs[:3]] + [outs[3].reshape(layers, depth, width)]
    return tuple(
        pl.pallas_call(
            write_out,
            out_shape=[jax.ShapeDtypeStruct(out.shape, out.dtype) for out in outs],
            in_specs=[pl.BlockSpec(memory_space=pltpu.VMEM)] * 4,
            out_specs=[anywhere] * 4,
            scratch_shapes=[dma((4, layers))],
            compiler_params=pltpu.CompilerParams(vmem_limit_bytes=16 * 1024 * 1024),
        )(*outs)
    )


def solution(mesh):
    fsdp, tp = mesh.shape["fsdp"], mesh.shape["tp"]
    local = plain
    if fsdp >= 4 and fsdp & (fsdp - 1) == 0 and tp > 1 and tp & (tp - 1) == 0:
        local = functools.partial(fused, fsdp, tp)
    in_specs = (
        P("fsdp", None, None, "tp"),
        P("fsdp"),
        P(),
        P(None, "fsdp", "tp"),
        P(None, "fsdp", "tp"),
        P(None, "fsdp", "tp"),
    )
    out_specs = (
        P(None, "fsdp", "tp"),
        P(None, "fsdp", "tp"),
        P(None, "fsdp", "tp"),
        P(None, None, "tp"),
    )
    return jax.shard_map(local, mesh=mesh, in_specs=in_specs, out_specs=out_specs, check_vma=False)
```

```python
import functools

import jax
import jax.numpy as jnp
from jax import lax
from jax.experimental import pallas as pl
from jax.experimental.pallas import tpu as pltpu
from jax.sharding import PartitionSpec as P

STEP = 10
MESH = pl.DeviceIdType.MESH
SPLIT = 10
TILE = 16
SPAN = 80
AHEAD = 2
LATE = 2
LEVELS = 127
FINE = LEVELS * 256


def plain(partials, token_counts, owner_map, params, moment1, moment2):
    weight = token_counts.astype(jnp.float32)[0]
    total = lax.psum(weight, "fsdp")
    summed = lax.psum_scatter(
        weight * partials[0].astype(jnp.float32), "fsdp", scatter_dimension=1, tiled=True
    )
    first, second, direction, new_params = adam(summed * (1.0 / total), params, moment1, moment2)
    delta = direction.astype(jnp.bfloat16)
    owners = lax.axis_size("tp")
    served = lax.dynamic_index_in_dim(owner_map, lax.axis_index("tp"), 1, keepdims=False)
    blocks = lax.all_gather(delta, "tp", axis=0)
    kept = jnp.take_along_axis(blocks, served[None, :, None, None], axis=0)[0]
    rollout = lax.all_gather(kept, "fsdp", axis=1, tiled=True)
    return (new_params, first, second, rollout)


def adam(grad, params, moment1, moment2):
    first = 0.9 * moment1 + 0.1 * grad
    second = 0.999 * moment2 + 0.001 * grad * grad
    scale_one = 1.0 / (1.0 - 0.9**STEP)
    scale_two = 1.0 / (1.0 - 0.999**STEP)
    direction = first * scale_one / (jnp.sqrt(second * scale_two) + 1e-08)
    new_params = params - 0.001 * (direction + 0.1 * params)
    return first, second, direction, new_params


def code(value, high):
    rest = jnp.where(high == 0.0, 0.0, (value - high) * FINE / high)
    return (rest + (LEVELS + 1.5)).astype(jnp.int32)


def decode(high, number):
    return high + (number.astype(jnp.float32) - (LEVELS + 1.0)) * (high * (1.0 / FINE))


def kernel(
    sizes,
    owner_ref,
    count_ref,
    part_ref,
    p_ref,
    m_ref,
    v_ref,
    np_ref,
    nm_ref,
    nv_ref,
    roll_ref,
    own_w,
    wbuf,
    mine,
    theirs,
    out_hi,
    out_lo,
    in_hi,
    in_lo,
    acc,
    held,
    cross,
    w_s,
    w_r,
    opt_s,
    ld_s,
    raw_s,
    raw_r,
    hi_s,
    hi_r,
    lo_s,
    lo_r,
    z_s,
    z_r,
    ag_s,
    ag_r,
    fin_s,
    fin_r,
):
    layers, fsdp, tp, parts, rows = sizes
    chunks = layers * parts
    pairs = fsdp // 2
    kept = pairs // 2
    bits = pairs.bit_length() - 1
    me = lax.axis_index("fsdp")
    col = lax.axis_index("tp")
    core = lax.rem(me, 2)
    mine_q = me // 2
    partner = mine_q * 2 + (1 - core)

    def away(index, flips):
        q = index
        for b in flips:
            q = q + (1 - 2 * lax.rem(index // (1 << b), 2)) * (1 << b)
        return q

    def ones(number):
        return [b for b in range(number.bit_length()) if number >> b & 1]

    tp_bits = tp.bit_length() - 1
    barrier = pltpu.get_barrier_semaphore()
    for d in range(1, fsdp):
        pl.semaphore_signal(
            barrier, inc=1, device_id={"fsdp": lax.rem(me + d, fsdp)}, device_id_type=MESH
        )
    for b in range(tp_bits):
        pl.semaphore_signal(
            barrier, inc=1, device_id={"tp": away(col, [b])}, device_id_type=MESH
        )

    def where(c):
        return c // parts, c % parts

    def order(c):
        names = list(range(bits))
        return names if c % 2 == 0 else names[::-1]

    def flipped(flips):
        return away(mine_q, flips)

    def block_of(c, pos):
        return flipped([order(c)[i] for i in range(bits) if pos >> (bits - 1 - i) & 1])

    own_w[...] = jnp.full(own_w.shape, count_ref[0], jnp.int32).astype(jnp.float32)
    loads = []
    for c in range(chunks):
        l, k = where(c)
        load = pltpu.make_async_copy(part_ref.at[l, :, core, k], mine.at[c], ld_s.at[c])
        load.start()
        loads.append(load)
    pl.semaphore_wait(barrier, fsdp - 1 + tp_bits)

    def push(src, dst, send, arrive, **device):
        copy = pltpu.make_async_remote_copy(
            src_ref=src,
            dst_ref=dst,
            send_sem=send,
            recv_sem=arrive,
            device_id=device,
            device_id_type=MESH,
        )
        copy.start()
        return copy

    weights = [None] * fsdp

    groups = [tuple(range(c, min(c + 2, chunks))) for c in range(0, chunks, 2)]
    for d in range(1, fsdp):
        weights[d] = push(own_w, wbuf.at[d], w_s.at[d], w_r.at[d], fsdp=lax.rem(me + d, fsdp))
    raws = []
    for c in range(chunks):
        l, k = where(c)
        raws.append(
            push(
                part_ref.at[l, :, 1 - core, k],
                theirs.at[c],
                raw_s.at[c],
                raw_r.at[c],
                fsdp=partner,
            )
        )
    opts = []
    for i, (src, dst) in enumerate(((p_ref, np_ref), (m_ref, nm_ref), (v_ref, nv_ref))):
        load = pltpu.make_async_copy(src, dst, opt_s.at[i])
        load.start()
        opts.append(load)

    lanes = own_w.shape[1]
    width = mine.shape[3]

    def row(tile):
        return jnp.concatenate([tile[0:1, :]] * (width // lanes), axis=1)

    my_weight = row(own_w[...])
    all_weights = []

    def weigh():
        total = my_weight
        for d in range(1, fsdp):
            weights[d].wait()
            total = total + row(wbuf[d])
        all_weights.append(row(wbuf[lax.rem(me - partner + fsdp, fsdp)]))
        all_weights.append(1.0 / total)

    side = rows // 2
    step = next(n for n in range(min(side, SPAN), 0, -TILE) if side % n == 0)

    def tiles(body):
        def run(i, carry):
            body(pl.ds(pl.multiple_of(i * step, step), step))
            return carry

        lax.fori_loop(0, rows // step, run, 0)

    def quads(body):
        def run(i, carry):
            start = pl.multiple_of(i * step, step)
            body(pl.ds(start, step), pl.ds(pl.multiple_of(start + side, step), step))
            return carry

        lax.fori_loop(0, side // step, run, 0)

    halving = {}
    spread = {}

    def halve(c, i):
        half = pairs >> (i + 1)
        there = flipped([order(c)[i]]) * 2 + core
        halving[c, i] = [
            push(
                src.at[c, pl.ds(half, half)],
                dst.at[c, pl.ds(half, half)],
                send.at[c, i],
                arrive.at[c, i],
                fsdp=there,
            )
            for src, dst, send, arrive in (
                (out_hi, in_hi, hi_s, hi_r),
                (out_lo, in_lo, lo_s, lo_r),
            )
        ]

    def arrived(c, i):
        for copy in halving[c, i]:
            copy.wait_recv()

    def pair_sum(c, pos, at):
        q = block_of(c, pos)
        return my_weight * mine[c, q, at, :].astype(jnp.float32) + all_weights[0] * theirs[
            c, q, at, :
        ].astype(jnp.float32)

    def write(c, pos, at, pair, values):
        numbers = []
        for rows_at, value in zip(pair, values):
            high = value.astype(jnp.bfloat16)
            out_hi[c, pos, rows_at, :] = high
            number = code(value, high.astype(jnp.float32))
            numbers += [number[:, : width // 2], number[:, width // 2 :]]
        word = numbers[0]
        for n in range(1, 4):
            word = word | (numbers[n] << (8 * n))
        out_lo[c, pos, at, :] = word

    def read(c, pos, at, pair):
        word = in_lo[c, pos, at, :]
        numbers = [(word >> (8 * n)) & 255 for n in range(4)]
        return [
            decode(
                in_hi[c, pos, rows_at, :].astype(jnp.float32),
                jnp.concatenate(numbers[2 * n : 2 * n + 2], axis=1),
            )
            for n, rows_at in enumerate(pair)
        ]

    def held_rows(c, pos):
        q = flipped([order(c)[b] for b in ones(pos)])
        l, k = where(c)
        return roll_ref.at[l, q, core, k]

    def double(c, j):
        there = flipped([order(c)[j]]) * 2 + core
        for pos in range(1 << j):
            block = held_rows(c, pos)
            push(block, block, ag_s.at[c, j], ag_r.at[c, j], fsdp=there)

    def await_part(part, sem):
        pltpu.make_async_copy(part, part, sem).wait()

    def await_blocks(c, count, sem):
        await_part(mine.at[c, pl.ds(0, count)], sem)

    def first_half(c):
        loads[c].wait()
        raws[c].wait_recv()
        if c == 0:
            weigh()
        for pos in range(pairs - 1, kept - 1, -1):

            def body(*pair):
                write(c, pos, pair[0], pair, [pair_sum(c, pos, at) for at in pair])

            quads(body)
        halve(c, 0)

    def add(i, c):
        arrived(c, i)
        half = pairs >> (i + 1)
        for pos in range(half - 1, -1, -1):

            def body(*pair):
                totals = read(c, half + pos, pair[0], pair)
                for n, at in enumerate(pair):
                    totals[n] += pair_sum(c, pos, at) if i == 0 else acc[c, pos, at, :]
                if half > 1 and pos >= half // 2:
                    write(c, pos, pair[0], pair, totals)
                else:
                    for at, total in zip(pair, totals):
                        acc[c, pos, at, :] = total

            quads(body)
            if half > 1 and pos == half // 2:
                halve(c, i + 1)

    def update(c):
        l, k = where(c)
        arrived(c, bits - 1)
        if c == 0:
            for load in opts:
                load.wait()
        scale = all_weights[1]

        def body(*pair):
            totals = read(c, 1, pair[0], pair)
            for at, total in zip(pair, totals):
                total = total + (pair_sum(c, 0, at) if bits == 1 else acc[c, 0, at, :])
                first, second, direction, new_params = adam(
                    total * scale, np_ref[l, k, at, :], nm_ref[l, k, at, :], nv_ref[l, k, at, :]
                )
                held[c, 0, at, :] = direction.astype(jnp.bfloat16)
                np_ref[l, k, at, :] = new_params
                nm_ref[l, k, at, :] = first
                nv_ref[l, k, at, :] = second

        quads(body)
        if tp_bits > 1:
            meet(c, 0)
        else:
            hand_over(c)

    def meet(c, b):
        size = 1 << b
        spread[c, b] = push(
            held.at[c, pl.ds(0, size)],
            held.at[c, pl.ds(size, size)],
            z_s.at[c, b],
            z_r.at[c, b],
            tp=away(col, [b]),
        )

    def pick(c, at, served, start):
        chosen = start
        for slot in range(tp // 2):
            chosen = jnp.where(
                served == away(col, ones(slot)), held[c, slot, at, :].astype(jnp.float32), chosen
            )
        return chosen.astype(jnp.bfloat16)

    def hand_over(c):
        l, k = where(c)
        there = away(col, [tp_bits - 1])
        served = owner_ref[l, there]

        def body(at):
            cross[c, 0, at, :] = pick(c, at, served, held[c, 0, at, :].astype(jnp.float32))

        tiles(body)
        spread[c, tp_bits - 1] = push(
            cross.at[c, 0],
            cross.at[c, 1],
            z_s.at[c, tp_bits - 1],
            z_r.at[c, tp_bits - 1],
            tp=there,
        )

    def met(b, c):
        spread[c, b].wait_recv()
        if b + 2 < tp_bits:
            meet(c, b + 1)
        else:
            hand_over(c)

    def select(c):
        l, k = where(c)
        spread[c, tp_bits - 1].wait_recv()
        served = owner_ref[l, col]

        def body(at):
            roll_ref[l, mine_q, core, k, at, :] = pick(
                c, at, served, cross[c, 1, at, :].astype(jnp.float32)
            )

        tiles(body)
        double(c, 0)
        finish(c, 0, 1)

    def finish(c, first, count):
        for pos in range(first, first + count):
            block = held_rows(c, pos)
            push(block, block, fin_s.at[c], fin_r.at[c], fsdp=partner)

    def forward(j, c):
        await_blocks(c, 1 << j, ag_r.at[c, j])
        if j + 1 < bits:
            double(c, j + 1)
        finish(c, 1 << j, 1 << j)

    stages = [first_half]
    lags = [0]
    middle = [functools.partial(add, i) for i in range(bits - 1)]
    middle += [update]
    middle += [functools.partial(met, b) for b in range(tp_bits - 1)]
    lags += [AHEAD + i for i in range(len(middle))]
    tail = [select] + [functools.partial(forward, j) for j in range(bits)]
    lags += [lags[-1] + 1 + LATE + i for i in range(len(tail))]
    stages += middle + tail
    for t in range(len(groups) + lags[-1]):
        for lag, stage in zip(lags, stages):
            if 0 <= t - lag < len(groups):
                for c in groups[t - lag]:
                    stage(c)

    for c in range(chunks):
        raws[c].wait_send()
        for i in range(bits):
            for copy in halving[c, i]:
                copy.wait_send()
            await_blocks(c, 1 << i, ag_s.at[c, i])
        for b in range(tp_bits):
            spread[c, b].wait_send()
        for sem in (fin_s, fin_r):
            await_part(roll_ref.at[0, :, 0, 0], sem.at[c])


def write_out(*refs):
    count = len(refs) // 2
    copies = []
    for i in range(count):
        for l in range(refs[i].shape[0]):
            sem = refs[-1].at[i, l]
            copies.append(pltpu.make_async_copy(refs[i].at[l], refs[count + i].at[l], sem))
    for copy in copies:
        copy.start()
    for copy in copies:
        copy.wait()


def fused(fsdp, tp, partials, token_counts, owner_map, params, moment1, moment2):
    layers, depth, width = partials.shape[1:]
    per = params.shape[1]
    if per % (2 * TILE) or width % 256:
        return plain(partials, token_counts, owner_map, params, moment1, moment2)
    pairs = fsdp // 2
    bits = pairs.bit_length() - 1
    tp_bits = tp.bit_length() - 1
    parts = next(n for n in range(SPLIT, 0, -1) if per % (n * 2 * TILE) == 0)
    rows = per // parts
    chunks = layers * parts
    lanes = 128
    anywhere = pl.BlockSpec(memory_space=pl.ANY)
    dma = pltpu.SemaphoreType.DMA
    state = (layers, parts, rows, width)
    f32, b16 = jnp.float32, jnp.bfloat16
    outs = pl.pallas_call(
        functools.partial(kernel, (layers, fsdp, tp, parts, rows)),
        out_shape=[
            pltpu.VMEM(state, f32),
            pltpu.VMEM(state, f32),
            pltpu.VMEM(state, f32),
            pltpu.VMEM((layers, pairs, 2, parts, rows, width), b16),
        ],
        in_specs=[
            pl.BlockSpec(memory_space=pltpu.SMEM),
            pl.BlockSpec(memory_space=pltpu.SMEM),
            anywhere,
            anywhere,
            anywhere,
            anywhere,
        ],
        out_specs=[pl.BlockSpec(memory_space=pltpu.VMEM)] * 4,
        scratch_shapes=[
            pltpu.VMEM((8, lanes), f32),
            pltpu.VMEM((fsdp, 8, lanes), f32),
            pltpu.VMEM((chunks, pairs, rows, width), b16),
            pltpu.VMEM((chunks, pairs, rows, width), b16),
            pltpu.VMEM((chunks, pairs, rows, width), b16),
            pltpu.VMEM((chunks, pairs, rows // 2, width // 2), jnp.int32),
            pltpu.VMEM((chunks, pairs, rows, width), b16),
            pltpu.VMEM((chunks, pairs, rows // 2, width // 2), jnp.int32),
            pltpu.VMEM((chunks, pairs // 2, rows, width), f32),
            pltpu.VMEM((chunks, tp // 2, rows, width), b16),
            pltpu.VMEM((chunks, 2, rows, width), b16),
            dma((fsdp,)),
            dma((fsdp,)),
            dma((3,)),
            dma((chunks,)),
            dma((chunks,)),
            dma((chunks,)),
            dma((chunks, bits)),
            dma((chunks, bits)),
            dma((chunks, bits)),
            dma((chunks, bits)),
            dma((chunks, tp_bits)),
            dma((chunks, tp_bits)),
            dma((chunks, bits)),
            dma((chunks, bits)),
            dma((chunks,)),
            dma((chunks,)),
        ],
        compiler_params=pltpu.CompilerParams(
            collective_id=0, has_side_effects=True, vmem_limit_bytes=48 * 1024 * 1024
        ),
    )(
        owner_map,
        token_counts,
        partials.reshape(layers, pairs, 2, parts, rows, width),
        params.reshape(state),
        moment1.reshape(state),
        moment2.reshape(state),
    )
    outs = [out.reshape(params.shape) for out in outs[:3]] + [outs[3].reshape(layers, depth, width)]
    return tuple(
        pl.pallas_call(
            write_out,
            out_shape=[jax.ShapeDtypeStruct(out.shape, out.dtype) for out in outs],
            in_specs=[pl.BlockSpec(memory_space=pltpu.VMEM)] * 4,
            out_specs=[anywhere] * 4,
            scratch_shapes=[dma((4, layers))],
            compiler_params=pltpu.CompilerParams(vmem_limit_bytes=16 * 1024 * 1024),
        )(*outs)
    )


def solution(mesh):
    fsdp, tp = mesh.shape["fsdp"], mesh.shape["tp"]
    local = plain
    if fsdp >= 4 and fsdp & (fsdp - 1) == 0 and tp > 1 and tp & (tp - 1) == 0:
        local = functools.partial(fused, fsdp, tp)
    in_specs = (
        P("fsdp", None, None, "tp"),
        P("fsdp"),
        P(),
        P(None, "fsdp", "tp"),
        P(None, "fsdp", "tp"),
        P(None, "fsdp", "tp"),
    )
    out_specs = (
        P(None, "fsdp", "tp"),
        P(None, "fsdp", "tp"),
        P(None, "fsdp", "tp"),
        P(None, None, "tp"),
    )
    return jax.shard_map(local, mesh=mesh, in_specs=in_specs, out_specs=out_specs, check_vma=False)
```

```python
import functools

import jax
import jax.numpy as jnp
from jax import lax
from jax.experimental import pallas as pl
from jax.experimental.pallas import tpu as pltpu
from jax.sharding import PartitionSpec as P

STEP = 10
MESH = pl.DeviceIdType.MESH
SPLIT = 20
TILE = 16
SPAN = 80
AHEAD = 3
LATE = 6
GAP = 3
ZGAP = 3
AGAP = 4
CUTS = 5
LEVELS = 127
FINE = LEVELS * 256


def plain(partials, token_counts, owner_map, params, moment1, moment2):
    weight = token_counts.astype(jnp.float32)[0]
    total = lax.psum(weight, "fsdp")
    summed = lax.psum_scatter(
        weight * partials[0].astype(jnp.float32), "fsdp", scatter_dimension=1, tiled=True
    )
    first, second, direction, new_params = adam(summed * (1.0 / total), params, moment1, moment2)
    delta = direction.astype(jnp.bfloat16)
    owners = lax.axis_size("tp")
    served = lax.dynamic_index_in_dim(owner_map, lax.axis_index("tp"), 1, keepdims=False)
    blocks = lax.all_gather(delta, "tp", axis=0)
    kept = jnp.take_along_axis(blocks, served[None, :, None, None], axis=0)[0]
    rollout = lax.all_gather(kept, "fsdp", axis=1, tiled=True)
    return (new_params, first, second, rollout)


def adam(grad, params, moment1, moment2):
    first = 0.9 * moment1 + 0.1 * grad
    second = 0.999 * moment2 + 0.001 * grad * grad
    scale_one = 1.0 / (1.0 - 0.9**STEP)
    scale_two = 1.0 / (1.0 - 0.999**STEP)
    direction = first * scale_one / (jnp.sqrt(second * scale_two) + 1e-08)
    new_params = params - 0.001 * (direction + 0.1 * params)
    return first, second, direction, new_params


def code(value, high):
    rest = jnp.where(high == 0.0, 0.0, (value - high) * FINE / high)
    return (rest + (LEVELS + 1.5)).astype(jnp.int32)


def decode(high, number):
    return high + (number.astype(jnp.float32) - (LEVELS + 1.0)) * (high * (1.0 / FINE))


def kernel(
    sizes,
    owner_hbm,
    count_hbm,
    part_ref,
    p_ref,
    m_ref,
    v_ref,
    np_ref,
    nm_ref,
    nv_ref,
    roll_ref,
    owner_ref,
    count_ref,
    own_w,
    scale,
    wbuf,
    mine,
    theirs,
    near,
    out_hi,
    out_lo,
    in_hi,
    in_lo,
    acc,
    held,
    cross,
    in_s,
    w_s,
    w_r,
    opt_s,
    ld_s,
    raw_s,
    raw_r,
    near_s,
    near_r,
    hi_s,
    lo_s,
    rs_r,
    z_s,
    z_r,
    ag_s,
    ag_r,
    fin_s,
    fin_r,
):
    layers, fsdp, tp, parts, rows = sizes
    chunks = layers * parts
    pairs = fsdp // 2
    kept = pairs // 2
    bits = pairs.bit_length() - 1
    me = lax.axis_index("fsdp")
    col = lax.axis_index("tp")
    core = lax.rem(me, 2)
    mine_q = me // 2
    partner = mine_q * 2 + (1 - core)

    def away(index, flips):
        q = index
        for b in flips:
            q = q + (1 - 2 * lax.rem(index // (1 << b), 2)) * (1 << b)
        return q

    def ones(number):
        return [b for b in range(number.bit_length()) if number >> b & 1]

    tp_bits = tp.bit_length() - 1
    barrier = pltpu.get_barrier_semaphore()
    for d in range(1, fsdp):
        pl.semaphore_signal(
            barrier, inc=1, device_id={"fsdp": lax.rem(me + d, fsdp)}, device_id_type=MESH
        )
    for b in range(tp_bits):
        pl.semaphore_signal(
            barrier, inc=1, device_id={"tp": away(col, [b])}, device_id_type=MESH
        )

    groups = chunks // 2
    width = mine.shape[3]
    lanes = own_w.shape[1]

    def where(c):
        return lax.div(c, parts), lax.rem(c, parts)

    def order(slot):
        names = list(range(bits))
        return names if slot == 0 else names[::-1]

    def flipped(flips):
        return away(mine_q, flips)

    def block_of(slot, pos):
        return flipped([order(slot)[i] for i in range(bits) if pos >> (bits - 1 - i) & 1])

    def repeat(count, body):
        def run(i, carry):
            body(i)
            return carry

        lax.fori_loop(0, count, run, 0)

    def fetch(c):
        l, k = where(c)
        pltpu.make_async_copy(part_ref.at[l, :, core, k], mine.at[c], ld_s.at[0]).start()

    count_copy = pltpu.make_async_copy(count_hbm, count_ref, in_s.at[0])
    count_copy.start()
    owner_copy = pltpu.make_async_copy(owner_hbm, owner_ref, in_s.at[1])
    owner_copy.start()
    repeat(chunks, fetch)
    opts = []
    for i, (src, dst) in enumerate(((p_ref, np_ref), (m_ref, nm_ref), (v_ref, nv_ref))):
        load = pltpu.make_async_copy(src, dst, opt_s.at[i])
        load.start()
        opts.append(load)
    count_copy.wait()
    own_w[...] = jnp.full(own_w.shape, count_ref[0], jnp.int32).astype(jnp.float32)
    pl.semaphore_wait(barrier, fsdp - 1 + tp_bits)

    def push(src, dst, send, arrive, **device):
        pltpu.make_async_remote_copy(
            src_ref=src,
            dst_ref=dst,
            send_sem=send,
            recv_sem=arrive,
            device_id=device,
            device_id_type=MESH,
        ).start()

    def await_part(part, sem):
        pltpu.make_async_copy(part, part, sem).wait()

    for slot in range(2):
        l, k = slot // parts, slot % parts
        there = flipped([order(slot)[0]]) * 2
        for pos in range(kept):
            for half in range(2):
                push(
                    part_ref.at[l, block_of(slot, kept + pos), half, k],
                    near.at[slot, core, pos],
                    near_s.at[0],
                    near_r.at[0],
                    fsdp=there + half,
                )

    def share(c):
        l, k = where(c)
        push(
            part_ref.at[l, :, 1 - core, k],
            theirs.at[c],
            raw_s.at[0],
            raw_r.at[lax.div(c, 2)],
            fsdp=partner,
        )

    repeat(chunks, share)
    for d in range(1, fsdp):
        push(own_w, wbuf.at[d], w_s.at[0], w_r.at[min(d - 1, 1)], fsdp=away(me, ones(d)))

    def row(tile):
        return jnp.concatenate([tile[0:1, :]] * (width // lanes), axis=1)

    def weigh():
        await_part(wbuf.at[pl.ds(2, fsdp - 2)], w_r.at[1])
        total = own_w[...]
        for d in range(1, fsdp):
            total = total + wbuf[d]
        scale[...] = 1.0 / total

    side = rows // 2
    step = next(n for n in range(min(side, SPAN), 0, -TILE) if side % n == 0)

    def tiles(body):
        for i in range(0, rows, step):
            body(pl.ds(i, step))

    def quads(body):
        for i in range(0, side, step):
            body(pl.ds(i, step), pl.ds(i + side, step))

    def both(body):
        def run(g):
            for slot in range(2):
                body(2 * g + slot, slot)

        return run

    def halve(c, slot, i):
        half = pairs >> (i + 1)
        there = flipped([order(slot)[i]]) * 2 + core
        for src, dst, send in ((out_hi, in_hi, hi_s), (out_lo, in_lo, lo_s)):
            push(
                src.at[c, pl.ds(half, half)],
                dst.at[c, pl.ds(half, half)],
                send.at[i],
                rs_r.at[lax.div(c, 2), i],
                fsdp=there,
            )

    def arrived(g, i):
        half = pairs >> (i + 1)
        tall, wide = (2, 3 * half // 2) if half > 1 else (3, 1)
        await_part(mine.at[pl.ds(0, tall), pl.ds(0, wide)], rs_r.at[g, i])

    def pair_sum(c, slot, pos, at):
        q = block_of(slot, pos)
        own = row(own_w[...]) * mine[c, q, at, :].astype(jnp.float32)
        return own + row(wbuf[1]) * theirs[c, q, at, :].astype(jnp.float32)

    def near_sum(slot, pos, at):
        index = 1 << (order(slot)[0] + 1)
        total = row(wbuf[index + core]) * near[slot, 0, pos, at, :].astype(jnp.float32)
        return total + row(wbuf[index + 1 - core]) * near[slot, 1, pos, at, :].astype(jnp.float32)

    def write(c, pos, at, pair, values):
        numbers = []
        for rows_at, value in zip(pair, values):
            high = value.astype(jnp.bfloat16)
            out_hi[c, pos, rows_at, :] = high
            number = code(value, high.astype(jnp.float32))
            numbers += [number[:, : width // 2], number[:, width // 2 :]]
        word = numbers[0]
        for n in range(1, 4):
            word = word | (numbers[n] << (8 * n))
        out_lo[c, pos, at, :] = word

    def read(c, pos, at, pair):
        word = in_lo[c, pos, at, :]
        numbers = [(word >> (8 * n)) & 255 for n in range(4)]
        return [
            decode(
                in_hi[c, pos, rows_at, :].astype(jnp.float32),
                jnp.concatenate(numbers[2 * n : 2 * n + 2], axis=1),
            )
            for n, rows_at in enumerate(pair)
        ]

    def held_rows(c, slot, pos):
        q = flipped([order(slot)[b] for b in ones(pos)])
        l, k = where(c)
        return roll_ref.at[l, q, core, k]

    def double(c, slot, j):
        there = flipped([order(slot)[j]]) * 2 + core
        for pos in range(1 << j):
            block = held_rows(c, slot, pos)
            push(block, block, ag_s.at[j], ag_r.at[lax.div(c, 2), j], fsdp=there)

    def pair_of(g):
        return pl.ds(2 * g, 2)

    def first_halves(g):
        await_part(theirs.at[pair_of(g)], raw_r.at[g])

        @pl.when(g == 0)
        def _():
            await_part(mine, ld_s.at[0])
            await_part(wbuf.at[1], w_r.at[0])

        @pl.when(g > 0)
        def _():
            both(first_half)(g)

    def first_half(c, slot):
        for pos in range(pairs - 1, kept - 1, -1):

            def body(*pair):
                write(c, pos, pair[0], pair, [pair_sum(c, slot, pos, at) for at in pair])

            quads(body)
        halve(c, slot, 0)

    def adds(i, g):
        if i > 0:
            arrived(g, i)
            both(functools.partial(add, i, False))(g)
            return

        @pl.when(g == 0)
        def _():
            await_part(near, near_r.at[0])
            weigh()
            both(functools.partial(add, i, True))(g)

        @pl.when(g > 0)
        def _():
            arrived(g, i)
            both(functools.partial(add, i, False))(g)

    def add(i, raw, c, slot):
        half = pairs >> (i + 1)
        for pos in range(half - 1, -1, -1):

            def body(*pair):
                if raw:
                    totals = [near_sum(slot, pos, at) for at in pair]
                else:
                    totals = read(c, half + pos, pair[0], pair)
                for n, at in enumerate(pair):
                    totals[n] += pair_sum(c, slot, pos, at) if i == 0 else acc[c, pos, at, :]
                if half > 1 and pos >= half // 2:
                    write(c, pos, pair[0], pair, totals)
                else:
                    for at, total in zip(pair, totals):
                        acc[c, pos, at, :] = total

            quads(body)
            if half > 1 and pos == half // 2:
                halve(c, slot, i + 1)

    def updates(g):
        @pl.when(g == 0)
        def _():
            for load in opts:
                load.wait()
            owner_copy.wait()

        arrived(g, bits - 1)
        both(update)(g)

    def update(c, slot):
        l, k = where(c)

        def body(*pair):
            totals = read(c, 1, pair[0], pair)
            for at, total in zip(pair, totals):
                total = total + acc[c, 0, at, :]
                first, second, direction, new_params = adam(
                    total * row(scale[...]),
                    np_ref[l, k, at, :],
                    nm_ref[l, k, at, :],
                    nv_ref[l, k, at, :],
                )
                held[c, 0, at, :] = direction.astype(jnp.bfloat16)
                np_ref[l, k, at, :] = new_params
                nm_ref[l, k, at, :] = first
                nv_ref[l, k, at, :] = second

        quads(body)
        if tp_bits > 1:
            meet(c, 0)
        else:
            hand_over(c, slot)

    def meet(c, b):
        size = 1 << b
        push(
            held.at[c, pl.ds(0, size)],
            held.at[c, pl.ds(size, size)],
            z_s.at[b],
            z_r.at[lax.div(c, 2), b],
            tp=away(col, [b]),
        )

    def pick(c, at, served, start):
        chosen = start
        for slot in range(tp // 2):
            chosen = jnp.where(
                served == away(col, ones(slot)), held[c, slot, at, :].astype(jnp.float32), chosen
            )
        return chosen.astype(jnp.bfloat16)

    def hand_over(c, slot):
        l, k = where(c)
        there = away(col, [tp_bits - 1])
        served = owner_ref[l, there]

        def body(at):
            cross[c, 0, at, :] = pick(c, at, served, held[c, 0, at, :].astype(jnp.float32))

        tiles(body)
        push(
            cross.at[c, 0],
            cross.at[c, 1],
            z_s.at[tp_bits - 1],
            z_r.at[lax.div(c, 2), tp_bits - 1],
            tp=there,
        )

    def met(b, g):
        size = 1 << b
        await_part(held.at[pair_of(g), pl.ds(size, size)], z_r.at[g, b])
        if b + 2 < tp_bits:
            for slot in range(2):
                meet(2 * g + slot, b + 1)
        else:
            both(hand_over)(g)

    def selects(g):
        await_part(cross.at[pair_of(g), 1], z_r.at[g, tp_bits - 1])
        both(select)(g)

    def select(c, slot):
        l, k = where(c)
        served = owner_ref[l, col]

        def body(at):
            roll_ref[l, mine_q, core, k, at, :] = pick(
                c, at, served, cross[c, 1, at, :].astype(jnp.float32)
            )

        tiles(body)
        double(c, slot, 0)
        finish(c, slot, 0, 1)

    def finish(c, slot, first, count):
        for pos in range(first, first + count):
            block = held_rows(c, slot, pos)
            push(block, block, fin_s.at[0], fin_r.at[0], fsdp=partner)

    def forward(j, g):
        await_part(mine.at[pl.ds(0, 2), pl.ds(0, 1 << j)], ag_r.at[g, j])
        for slot in range(2):
            if j + 1 < bits:
                double(2 * g + slot, slot, j + 1)
            finish(2 * g + slot, slot, 1 << j, 1 << j)

    stages = [first_halves]
    lags = [0]
    middle = [functools.partial(adds, i) for i in range(bits - 1)]
    middle += [updates]
    middle += [functools.partial(met, b) for b in range(tp_bits - 1)]
    lags += [AHEAD + GAP * i for i in range(bits)]
    lags += [lags[-1] + ZGAP * (b + 1) for b in range(tp_bits - 1)]
    tail = [selects] + [functools.partial(forward, j) for j in range(bits)]
    lags += [lags[-1] + LATE + AGAP * i for i in range(len(tail))]
    stages += middle + tail

    def at_step(t):
        for lag, stage in zip(lags, stages):
            g = t - lag
            pl.when(jnp.logical_and(g >= 0, g < groups))(functools.partial(stage, g))

    repeat(groups + lags[-1], at_step)

    await_part(wbuf.at[pl.ds(1, fsdp - 1)], w_s.at[0])
    await_part(theirs, raw_s.at[0])
    await_part(near, near_s.at[0])
    for i in range(bits):
        half = pairs >> (i + 1)
        sent = chunks if i > 0 else chunks - 2
        await_part(out_hi.at[pl.ds(0, sent), pl.ds(0, half)], hi_s.at[i])
        await_part(out_lo.at[pl.ds(0, sent), pl.ds(0, half)], lo_s.at[i])
        await_part(mine.at[:, pl.ds(0, 1 << i)], ag_s.at[i])
    for b in range(tp_bits - 1):
        await_part(held.at[:, pl.ds(0, 1 << b)], z_s.at[b])
    await_part(cross.at[:, 0], z_s.at[tp_bits - 1])
    for sem in (fin_s, fin_r):
        await_part(mine, sem.at[0])


def write_out(*refs):
    count = len(refs) // 2
    copies = []
    for i in range(count):
        n = refs[i].shape[1] // CUTS
        for l in range(refs[i].shape[0]):
            for j in range(CUTS):
                at = (l, pl.ds(j * n, n))
                copies.append(
                    pltpu.make_async_copy(refs[i].at[at], refs[count + i].at[at], refs[-1].at[i])
                )
    for copy in copies:
        copy.start()
    for i in range(count):
        pltpu.make_async_copy(refs[i], refs[count + i], refs[-1].at[i]).wait()


def fused(fsdp, tp, partials, token_counts, owner_map, params, moment1, moment2):
    layers, depth, width = partials.shape[1:]
    per = params.shape[1]
    pairs = fsdp // 2
    bits = pairs.bit_length() - 1
    tp_bits = tp.bit_length() - 1
    parts = next((n for n in range(SPLIT, 0, -1) if per % (n * 2 * TILE) == 0), None)
    if parts is None or width % 256 or layers * parts % 2 or layers * parts < 4:
        return plain(partials, token_counts, owner_map, params, moment1, moment2)
    rows = per // parts
    chunks = layers * parts
    lanes = 128
    anywhere = pl.BlockSpec(memory_space=pl.ANY)
    dma = pltpu.SemaphoreType.DMA
    state = (layers, parts, rows, width)
    f32, b16 = jnp.float32, jnp.bfloat16
    outs = pl.pallas_call(
        functools.partial(kernel, (layers, fsdp, tp, parts, rows)),
        out_shape=[
            pltpu.VMEM(state, f32),
            pltpu.VMEM(state, f32),
            pltpu.VMEM(state, f32),
            pltpu.VMEM((layers, pairs, 2, parts, rows, width), b16),
        ],
        in_specs=[
            anywhere,
            anywhere,
            anywhere,
            anywhere,
            anywhere,
            anywhere,
        ],
        out_specs=[pl.BlockSpec(memory_space=pltpu.VMEM)] * 4,
        scratch_shapes=[
            pltpu.SMEM((layers, tp), jnp.int32),
            pltpu.SMEM((1,), jnp.int32),
            pltpu.VMEM((8, lanes), f32),
            pltpu.VMEM((8, lanes), f32),
            pltpu.VMEM((fsdp, 8, lanes), f32),
            pltpu.VMEM((chunks, pairs, rows, width), b16),
            pltpu.VMEM((chunks, pairs, rows, width), b16),
            pltpu.VMEM((2, 2, pairs // 2, rows, width), b16),
            pltpu.VMEM((chunks, pairs, rows, width), b16),
            pltpu.VMEM((chunks, pairs, rows // 2, width // 2), jnp.int32),
            pltpu.VMEM((chunks, pairs, rows, width), b16),
            pltpu.VMEM((chunks, pairs, rows // 2, width // 2), jnp.int32),
            pltpu.VMEM((chunks, pairs // 2, rows, width), f32),
            pltpu.VMEM((chunks, tp // 2, rows, width), b16),
            pltpu.VMEM((chunks, 2, rows, width), b16),
            dma((2,)),
            dma((1,)),
            dma((2,)),
            dma((3,)),
            dma((1,)),
            dma((1,)),
            dma((chunks // 2,)),
            dma((1,)),
            dma((1,)),
            dma((bits,)),
            dma((bits,)),
            dma((chunks // 2, bits)),
            dma((tp_bits,)),
            dma((chunks // 2, tp_bits)),
            dma((bits,)),
            dma((chunks // 2, bits)),
            dma((1,)),
            dma((1,)),
        ],
        compiler_params=pltpu.CompilerParams(
            collective_id=0, has_side_effects=True, vmem_limit_bytes=48 * 1024 * 1024
        ),
    )(
        owner_map,
        token_counts,
        partials.reshape(layers, pairs, 2, parts, rows, width),
        params.reshape(state),
        moment1.reshape(state),
        moment2.reshape(state),
    )
    outs = [out.reshape(params.shape) for out in outs[:3]] + [outs[3].reshape(layers, depth, width)]
    return tuple(
        pl.pallas_call(
            write_out,
            out_shape=[jax.ShapeDtypeStruct(out.shape, out.dtype) for out in outs],
            in_specs=[pl.BlockSpec(memory_space=pltpu.VMEM)] * 4,
            out_specs=[anywhere] * 4,
            scratch_shapes=[dma((4,))],
            compiler_params=pltpu.CompilerParams(vmem_limit_bytes=16 * 1024 * 1024),
        )(*outs)
    )


def solution(mesh):
    fsdp, tp = mesh.shape["fsdp"], mesh.shape["tp"]
    local = plain
    if fsdp >= 8 and fsdp & (fsdp - 1) == 0 and tp > 1 and tp & (tp - 1) == 0:
        local = functools.partial(fused, fsdp, tp)
    in_specs = (
        P("fsdp", None, None, "tp"),
        P("fsdp"),
        P(),
        P(None, "fsdp", "tp"),
        P(None, "fsdp", "tp"),
        P(None, "fsdp", "tp"),
    )
    out_specs = (
        P(None, "fsdp", "tp"),
        P(None, "fsdp", "tp"),
        P(None, "fsdp", "tp"),
        P(None, None, "tp"),
    )
    return jax.shard_map(local, mesh=mesh, in_specs=in_specs, out_specs=out_specs, check_vma=False)
```

```python
import functools

import jax
import jax.numpy as jnp
from jax import lax
from jax.experimental import pallas as pl
from jax.experimental.pallas import tpu as pltpu
from jax.sharding import PartitionSpec as P

STEP = 10
MESH = pl.DeviceIdType.MESH
SPLIT = 20
TILE = 16
SPAN = 80
AHEAD = 3
LATE = 6
GAP = 3
ZGAP = 3
AGAP = 4
CUTS = 5
OCTAVES = 40
CODES = 1 << 19
FINE = CODES / OCTAVES
LARGEST = 12


def plain(partials, token_counts, owner_map, params, moment1, moment2):
    weight = token_counts.astype(jnp.float32)[0]
    total = lax.psum(weight, "fsdp")
    summed = lax.psum_scatter(
        weight * partials[0].astype(jnp.float32), "fsdp", scatter_dimension=1, tiled=True
    )
    first, second, direction, new_params = adam(summed * (1.0 / total), params, moment1, moment2)
    delta = direction.astype(jnp.bfloat16)
    owners = lax.axis_size("tp")
    served = lax.dynamic_index_in_dim(owner_map, lax.axis_index("tp"), 1, keepdims=False)
    blocks = lax.all_gather(delta, "tp", axis=0)
    kept = jnp.take_along_axis(blocks, served[None, :, None, None], axis=0)[0]
    rollout = lax.all_gather(kept, "fsdp", axis=1, tiled=True)
    return (new_params, first, second, rollout)


def adam(grad, params, moment1, moment2):
    first = 0.9 * moment1 + 0.1 * grad
    second = 0.999 * moment2 + 0.001 * grad * grad
    scale_one = 1.0 / (1.0 - 0.9**STEP)
    scale_two = 1.0 / (1.0 - 0.999**STEP)
    direction = first * scale_one / (jnp.sqrt(second * scale_two) + 1e-08)
    new_params = params - 0.001 * (direction + 0.1 * params)
    return first, second, direction, new_params


def code(value, top):
    level = (jnp.log2(jnp.abs(value)) + (OCTAVES - top)) * FINE
    number = (jnp.clip(level, 0.0, CODES - 1.0) + 0.5).astype(jnp.int32)
    return jnp.where(value < 0.0, number + CODES, number)


def decode(number, top):
    level = number & (CODES - 1)
    size = jnp.exp2(level.astype(jnp.float32) * (1.0 / FINE) - (OCTAVES - top))
    size = jnp.where(level == 0, 0.0, size)
    return jnp.where(number >= CODES, -size, size)


def kernel(
    sizes,
    owner_hbm,
    count_hbm,
    part_ref,
    p_ref,
    m_ref,
    v_ref,
    np_ref,
    nm_ref,
    nv_ref,
    roll_ref,
    owner_ref,
    count_ref,
    own_w,
    scale,
    wbuf,
    mine,
    theirs,
    near,
    out_hi,
    out_lo,
    in_hi,
    in_lo,
    acc,
    held,
    cross,
    in_s,
    w_s,
    w_r,
    opt_s,
    ld_s,
    raw_s,
    raw_r,
    near_s,
    near_r,
    hi_s,
    lo_s,
    rs_r,
    z_s,
    z_r,
    ag_s,
    ag_r,
    fin_s,
    fin_r,
):
    layers, fsdp, tp, parts, rows = sizes
    chunks = layers * parts
    pairs = fsdp // 2
    kept = pairs // 2
    bits = pairs.bit_length() - 1
    me = lax.axis_index("fsdp")
    col = lax.axis_index("tp")
    core = lax.rem(me, 2)
    mine_q = me // 2
    partner = mine_q * 2 + (1 - core)

    def away(index, flips):
        q = index
        for b in flips:
            q = q + (1 - 2 * lax.rem(index // (1 << b), 2)) * (1 << b)
        return q

    def ones(number):
        return [b for b in range(number.bit_length()) if number >> b & 1]

    tp_bits = tp.bit_length() - 1
    barrier = pltpu.get_barrier_semaphore()
    for d in range(1, fsdp):
        pl.semaphore_signal(
            barrier, inc=1, device_id={"fsdp": lax.rem(me + d, fsdp)}, device_id_type=MESH
        )
    for b in range(tp_bits):
        pl.semaphore_signal(
            barrier, inc=1, device_id={"tp": away(col, [b])}, device_id_type=MESH
        )

    groups = chunks // 2
    top = LARGEST + fsdp.bit_length() - 1
    width = mine.shape[3]
    lanes = own_w.shape[1]

    def where(c):
        return lax.div(c, parts), lax.rem(c, parts)

    def order(slot):
        names = list(range(bits))
        return names if slot == 0 else names[::-1]

    def flipped(flips):
        return away(mine_q, flips)

    def block_of(slot, pos):
        return flipped([order(slot)[i] for i in range(bits) if pos >> (bits - 1 - i) & 1])

    def repeat(count, body):
        def run(i, carry):
            body(i)
            return carry

        lax.fori_loop(0, count, run, 0)

    def fetch(c):
        l, k = where(c)
        pltpu.make_async_copy(part_ref.at[l, :, core, k], mine.at[c], ld_s.at[0]).start()

    count_copy = pltpu.make_async_copy(count_hbm, count_ref, in_s.at[0])
    count_copy.start()
    owner_copy = pltpu.make_async_copy(owner_hbm, owner_ref, in_s.at[1])
    owner_copy.start()
    repeat(chunks, fetch)
    opts = []
    for i, (src, dst) in enumerate(((p_ref, np_ref), (m_ref, nm_ref), (v_ref, nv_ref))):
        load = pltpu.make_async_copy(src, dst, opt_s.at[i])
        load.start()
        opts.append(load)
    count_copy.wait()
    own_w[...] = jnp.full(own_w.shape, count_ref[0], jnp.int32).astype(jnp.float32)
    pl.semaphore_wait(barrier, fsdp - 1 + tp_bits)

    def push(src, dst, send, arrive, **device):
        pltpu.make_async_remote_copy(
            src_ref=src,
            dst_ref=dst,
            send_sem=send,
            recv_sem=arrive,
            device_id=device,
            device_id_type=MESH,
        ).start()

    def await_part(part, sem):
        pltpu.make_async_copy(part, part, sem).wait()

    for slot in range(2):
        l, k = slot // parts, slot % parts
        there = flipped([order(slot)[0]]) * 2
        for pos in range(kept):
            for half in range(2):
                push(
                    part_ref.at[l, block_of(slot, kept + pos), half, k],
                    near.at[slot, core, pos],
                    near_s.at[0],
                    near_r.at[0],
                    fsdp=there + half,
                )

    def share(c):
        l, k = where(c)
        push(
            part_ref.at[l, :, 1 - core, k],
            theirs.at[c],
            raw_s.at[0],
            raw_r.at[lax.div(c, 2)],
            fsdp=partner,
        )

    repeat(chunks, share)
    for d in range(1, fsdp):
        push(own_w, wbuf.at[d], w_s.at[0], w_r.at[min(d - 1, 1)], fsdp=away(me, ones(d)))

    def row(tile):
        return jnp.concatenate([tile[0:1, :]] * (width // lanes), axis=1)

    def weigh():
        await_part(wbuf.at[pl.ds(2, fsdp - 2)], w_r.at[1])
        total = own_w[...]
        for d in range(1, fsdp):
            total = total + wbuf[d]
        scale[...] = 1.0 / total

    side = rows // 2
    step = next(n for n in range(min(side, SPAN), 0, -TILE) if side % n == 0)

    def tiles(body):
        for i in range(0, rows, step):
            body(pl.ds(i, step))

    def quads(body):
        for i in range(0, side, step):
            body(pl.ds(i, step), pl.ds(i + side, step))

    def both(body):
        def run(g):
            for slot in range(2):
                body(2 * g + slot, slot)

        return run

    def halve(c, slot, i):
        half = pairs >> (i + 1)
        there = flipped([order(slot)[i]]) * 2 + core
        for src, dst, send in ((out_hi, in_hi, hi_s), (out_lo, in_lo, lo_s)):
            push(
                src.at[c, pl.ds(half, half)],
                dst.at[c, pl.ds(half, half)],
                send.at[i],
                rs_r.at[lax.div(c, 2), i],
                fsdp=there,
            )

    def arrived(g, i):
        half = pairs >> (i + 1)
        await_part(in_lo.at[pl.ds(0, 5), pl.ds(0, 2 * half)], rs_r.at[g, i])

    def pair_sum(c, slot, pos, at):
        q = block_of(slot, pos)
        own = row(own_w[...]) * mine[c, q, at, :].astype(jnp.float32)
        return own + row(wbuf[1]) * theirs[c, q, at, :].astype(jnp.float32)

    def near_sum(slot, pos, at):
        index = 1 << (order(slot)[0] + 1)
        total = row(wbuf[index + core]) * near[slot, 0, pos, at, :].astype(jnp.float32)
        return total + row(wbuf[index + 1 - core]) * near[slot, 1, pos, at, :].astype(jnp.float32)

    def fine_rows(at):
        return pl.ds(at.start // 2, at.size // 2)

    def write(c, pos, pair, values):
        numbers = [code(value, top) for value in values]
        out_hi[c, pos, pair[0], :] = (numbers[0] >> 4) | ((numbers[1] >> 4) << 16)
        middle, half = step // 2, width // 2
        word = None
        for n, number in enumerate(numbers):
            low = number & 15
            low = low[:middle] | (low[middle:] << 4)
            low = (low[:, :half] | (low[:, half:] << 8)) << (16 * n)
            word = low if word is None else word | low
        out_lo[c, pos, fine_rows(pair[0]), :] = word

    def read(c, pos, pair):
        high = in_hi[c, pos, pair[0], :]
        word = in_lo[c, pos, fine_rows(pair[0]), :]
        values = []
        for n in range(2):
            low = (word >> (16 * n)) & 65535
            low = jnp.concatenate([low & 255, low >> 8], axis=1)
            low = jnp.concatenate([low & 15, low >> 4], axis=0)
            values.append(decode((((high >> (16 * n)) & 65535) << 4) | low, top))
        return values

    def held_rows(c, slot, pos):
        q = flipped([order(slot)[b] for b in ones(pos)])
        l, k = where(c)
        return roll_ref.at[l, q, core, k]

    def double(c, slot, j):
        there = flipped([order(slot)[j]]) * 2 + core
        for pos in range(1 << j):
            block = held_rows(c, slot, pos)
            push(block, block, ag_s.at[j], ag_r.at[lax.div(c, 2), j], fsdp=there)

    def pair_of(g):
        return pl.ds(2 * g, 2)

    def first_halves(g):
        await_part(theirs.at[pair_of(g)], raw_r.at[g])

        @pl.when(g == 0)
        def _():
            await_part(mine, ld_s.at[0])
            await_part(wbuf.at[1], w_r.at[0])

        @pl.when(g > 0)
        def _():
            both(first_half)(g)

    def first_half(c, slot):
        for pos in range(pairs - 1, kept - 1, -1):

            def body(*pair):
                write(c, pos, pair, [pair_sum(c, slot, pos, at) for at in pair])

            quads(body)
        halve(c, slot, 0)

    def adds(i, g):
        if i > 0:
            arrived(g, i)
            both(functools.partial(add, i, False))(g)
            return

        @pl.when(g == 0)
        def _():
            await_part(near, near_r.at[0])
            weigh()
            both(functools.partial(add, i, True))(g)

        @pl.when(g > 0)
        def _():
            arrived(g, i)
            both(functools.partial(add, i, False))(g)

    def add(i, raw, c, slot):
        half = pairs >> (i + 1)
        for pos in range(half - 1, -1, -1):

            def body(*pair):
                if raw:
                    totals = [near_sum(slot, pos, at) for at in pair]
                else:
                    totals = read(c, half + pos, pair)
                for n, at in enumerate(pair):
                    totals[n] += pair_sum(c, slot, pos, at) if i == 0 else acc[c, pos, at, :]
                if half > 1 and pos >= half // 2:
                    write(c, pos, pair, totals)
                else:
                    for at, total in zip(pair, totals):
                        acc[c, pos, at, :] = total

            quads(body)
            if half > 1 and pos == half // 2:
                halve(c, slot, i + 1)

    def updates(g):
        @pl.when(g == 0)
        def _():
            for load in opts:
                load.wait()
            owner_copy.wait()

        arrived(g, bits - 1)
        both(update)(g)

    def update(c, slot):
        l, k = where(c)

        def body(*pair):
            totals = read(c, 1, pair)
            for at, total in zip(pair, totals):
                total = total + acc[c, 0, at, :]
                first, second, direction, new_params = adam(
                    total * row(scale[...]),
                    np_ref[l, k, at, :],
                    nm_ref[l, k, at, :],
                    nv_ref[l, k, at, :],
                )
                held[c, 0, at, :] = direction.astype(jnp.bfloat16)
                np_ref[l, k, at, :] = new_params
                nm_ref[l, k, at, :] = first
                nv_ref[l, k, at, :] = second

        quads(body)
        if tp_bits > 1:
            meet(c, 0)
        else:
            hand_over(c, slot)

    def meet(c, b):
        size = 1 << b
        push(
            held.at[c, pl.ds(0, size)],
            held.at[c, pl.ds(size, size)],
            z_s.at[b],
            z_r.at[lax.div(c, 2), b],
            tp=away(col, [b]),
        )

    def pick(c, at, served, start):
        chosen = start
        for slot in range(tp // 2):
            chosen = jnp.where(
                served == away(col, ones(slot)), held[c, slot, at, :].astype(jnp.float32), chosen
            )
        return chosen.astype(jnp.bfloat16)

    def hand_over(c, slot):
        l, k = where(c)
        there = away(col, [tp_bits - 1])
        served = owner_ref[l, there]

        def body(at):
            cross[c, 0, at, :] = pick(c, at, served, held[c, 0, at, :].astype(jnp.float32))

        tiles(body)
        push(
            cross.at[c, 0],
            cross.at[c, 1],
            z_s.at[tp_bits - 1],
            z_r.at[lax.div(c, 2), tp_bits - 1],
            tp=there,
        )

    def met(b, g):
        size = 1 << b
        await_part(held.at[pair_of(g), pl.ds(size, size)], z_r.at[g, b])
        if b + 2 < tp_bits:
            for slot in range(2):
                meet(2 * g + slot, b + 1)
        else:
            both(hand_over)(g)

    def selects(g):
        await_part(cross.at[pair_of(g), 1], z_r.at[g, tp_bits - 1])
        both(select)(g)

    def select(c, slot):
        l, k = where(c)
        served = owner_ref[l, col]

        def body(at):
            roll_ref[l, mine_q, core, k, at, :] = pick(
                c, at, served, cross[c, 1, at, :].astype(jnp.float32)
            )

        tiles(body)
        double(c, slot, 0)
        finish(c, slot, 0, 1)

    def finish(c, slot, first, count):
        for pos in range(first, first + count):
            block = held_rows(c, slot, pos)
            push(block, block, fin_s.at[0], fin_r.at[0], fsdp=partner)

    def forward(j, g):
        await_part(mine.at[pl.ds(0, 2), pl.ds(0, 1 << j)], ag_r.at[g, j])
        for slot in range(2):
            if j + 1 < bits:
                double(2 * g + slot, slot, j + 1)
            finish(2 * g + slot, slot, 1 << j, 1 << j)

    stages = [first_halves]
    lags = [0]
    middle = [functools.partial(adds, i) for i in range(bits - 1)]
    middle += [updates]
    middle += [functools.partial(met, b) for b in range(tp_bits - 1)]
    lags += [AHEAD + GAP * i for i in range(bits)]
    lags += [lags[-1] + ZGAP * (b + 1) for b in range(tp_bits - 1)]
    tail = [selects] + [functools.partial(forward, j) for j in range(bits)]
    lags += [lags[-1] + LATE + AGAP * i for i in range(len(tail))]
    stages += middle + tail

    def at_step(t):
        for lag, stage in zip(lags, stages):
            g = t - lag
            pl.when(jnp.logical_and(g >= 0, g < groups))(functools.partial(stage, g))

    repeat(groups + lags[-1], at_step)

    await_part(wbuf.at[pl.ds(1, fsdp - 1)], w_s.at[0])
    await_part(theirs, raw_s.at[0])
    await_part(near, near_s.at[0])
    for i in range(bits):
        half = pairs >> (i + 1)
        sent = chunks if i > 0 else chunks - 2
        await_part(out_hi.at[pl.ds(0, sent), pl.ds(0, half)], hi_s.at[i])
        await_part(out_lo.at[pl.ds(0, sent), pl.ds(0, half)], lo_s.at[i])
        await_part(mine.at[:, pl.ds(0, 1 << i)], ag_s.at[i])
    for b in range(tp_bits - 1):
        await_part(held.at[:, pl.ds(0, 1 << b)], z_s.at[b])
    await_part(cross.at[:, 0], z_s.at[tp_bits - 1])
    for sem in (fin_s, fin_r):
        await_part(mine, sem.at[0])


def write_out(*refs):
    count = len(refs) // 2
    copies = []
    for i in range(count):
        n = refs[i].shape[1] // CUTS
        for l in range(refs[i].shape[0]):
            for j in range(CUTS):
                at = (l, pl.ds(j * n, n))
                copies.append(
                    pltpu.make_async_copy(refs[i].at[at], refs[count + i].at[at], refs[-1].at[i])
                )
    for copy in copies:
        copy.start()
    for i in range(count):
        pltpu.make_async_copy(refs[i], refs[count + i], refs[-1].at[i]).wait()


def fused(fsdp, tp, partials, token_counts, owner_map, params, moment1, moment2):
    layers, depth, width = partials.shape[1:]
    per = params.shape[1]
    pairs = fsdp // 2
    bits = pairs.bit_length() - 1
    tp_bits = tp.bit_length() - 1
    parts = next((n for n in range(SPLIT, 0, -1) if per % (n * 2 * TILE) == 0), None)
    if parts is None or width % 256 or layers * parts % 2 or layers * parts < 5:
        return plain(partials, token_counts, owner_map, params, moment1, moment2)
    rows = per // parts
    chunks = layers * parts
    lanes = 128
    anywhere = pl.BlockSpec(memory_space=pl.ANY)
    dma = pltpu.SemaphoreType.DMA
    state = (layers, parts, rows, width)
    f32, b16 = jnp.float32, jnp.bfloat16
    outs = pl.pallas_call(
        functools.partial(kernel, (layers, fsdp, tp, parts, rows)),
        out_shape=[
            pltpu.VMEM(state, f32),
            pltpu.VMEM(state, f32),
            pltpu.VMEM(state, f32),
            pltpu.VMEM((layers, pairs, 2, parts, rows, width), b16),
        ],
        in_specs=[
            anywhere,
            anywhere,
            anywhere,
            anywhere,
            anywhere,
            anywhere,
        ],
        out_specs=[pl.BlockSpec(memory_space=pltpu.VMEM)] * 4,
        scratch_shapes=[
            pltpu.SMEM((layers, tp), jnp.int32),
            pltpu.SMEM((1,), jnp.int32),
            pltpu.VMEM((8, lanes), f32),
            pltpu.VMEM((8, lanes), f32),
            pltpu.VMEM((fsdp, 8, lanes), f32),
            pltpu.VMEM((chunks, pairs, rows, width), b16),
            pltpu.VMEM((chunks, pairs, rows, width), b16),
            pltpu.VMEM((2, 2, pairs // 2, rows, width), b16),
            pltpu.VMEM((chunks, pairs, rows // 2, width), jnp.int32),
            pltpu.VMEM((chunks, pairs, rows // 4, width // 2), jnp.int32),
            pltpu.VMEM((chunks, pairs, rows // 2, width), jnp.int32),
            pltpu.VMEM((chunks, pairs, rows // 4, width // 2), jnp.int32),
            pltpu.VMEM((chunks, pairs // 2, rows, width), f32),
            pltpu.VMEM((chunks, tp // 2, rows, width), b16),
            pltpu.VMEM((chunks, 2, rows, width), b16),
            dma((2,)),
            dma((1,)),
            dma((2,)),
            dma((3,)),
            dma((1,)),
            dma((1,)),
            dma((chunks // 2,)),
            dma((1,)),
            dma((1,)),
            dma((bits,)),
            dma((bits,)),
            dma((chunks // 2, bits)),
            dma((tp_bits,)),
            dma((chunks // 2, tp_bits)),
            dma((bits,)),
            dma((chunks // 2, bits)),
            dma((1,)),
            dma((1,)),
        ],
        compiler_params=pltpu.CompilerParams(
            collective_id=0, has_side_effects=True, vmem_limit_bytes=48 * 1024 * 1024
        ),
    )(
        owner_map,
        token_counts,
        partials.reshape(layers, pairs, 2, parts, rows, width),
        params.reshape(state),
        moment1.reshape(state),
        moment2.reshape(state),
    )
    outs = [out.reshape(params.shape) for out in outs[:3]] + [outs[3].reshape(layers, depth, width)]
    return tuple(
        pl.pallas_call(
            write_out,
            out_shape=[jax.ShapeDtypeStruct(out.shape, out.dtype) for out in outs],
            in_specs=[pl.BlockSpec(memory_space=pltpu.VMEM)] * 4,
            out_specs=[anywhere] * 4,
            scratch_shapes=[dma((4,))],
            compiler_params=pltpu.CompilerParams(vmem_limit_bytes=16 * 1024 * 1024),
        )(*outs)
    )


def solution(mesh):
    fsdp, tp = mesh.shape["fsdp"], mesh.shape["tp"]
    local = plain
    if fsdp >= 8 and fsdp & (fsdp - 1) == 0 and tp > 1 and tp & (tp - 1) == 0:
        local = functools.partial(fused, fsdp, tp)
    in_specs = (
        P("fsdp", None, None, "tp"),
        P("fsdp"),
        P(),
        P(None, "fsdp", "tp"),
        P(None, "fsdp", "tp"),
        P(None, "fsdp", "tp"),
    )
    out_specs = (
        P(None, "fsdp", "tp"),
        P(None, "fsdp", "tp"),
        P(None, "fsdp", "tp"),
        P(None, None, "tp"),
    )
    return jax.shard_map(local, mesh=mesh, in_specs=in_specs, out_specs=out_specs, check_vma=False)
```

```python
import functools

import jax
import jax.numpy as jnp
from jax import lax
from jax.experimental import pallas as pl
from jax.experimental.pallas import tpu as pltpu
from jax.sharding import PartitionSpec as P

STEP = 10
MESH = pl.DeviceIdType.MESH
SPLIT = 20
TILE = 16
SPAN = 80
AHEAD = 3
LATE = 6
GAP = 3
ZGAP = 3
AGAP = 4
CUTS = 5
OCTAVES = 36
CODES = 1 << 19
FINE = CODES / OCTAVES
LARGEST = 12


def plain(partials, token_counts, owner_map, params, moment1, moment2):
    weight = token_counts.astype(jnp.float32)[0]
    total = lax.psum(weight, "fsdp")
    summed = lax.psum_scatter(
        weight * partials[0].astype(jnp.float32), "fsdp", scatter_dimension=1, tiled=True
    )
    first, second, direction, new_params = adam(summed * (1.0 / total), params, moment1, moment2)
    delta = direction.astype(jnp.bfloat16)
    owners = lax.axis_size("tp")
    served = lax.dynamic_index_in_dim(owner_map, lax.axis_index("tp"), 1, keepdims=False)
    blocks = lax.all_gather(delta, "tp", axis=0)
    kept = jnp.take_along_axis(blocks, served[None, :, None, None], axis=0)[0]
    rollout = lax.all_gather(kept, "fsdp", axis=1, tiled=True)
    return (new_params, first, second, rollout)


def adam(grad, params, moment1, moment2):
    first = 0.9 * moment1 + 0.1 * grad
    second = 0.999 * moment2 + 0.001 * grad * grad
    scale_one = 1.0 / (1.0 - 0.9**STEP)
    scale_two = 1.0 / (1.0 - 0.999**STEP)
    direction = first * scale_one / (jnp.sqrt(second * scale_two) + 1e-08)
    new_params = params - 0.001 * (direction + 0.1 * params)
    return first, second, direction, new_params


def code(value, top):
    level = (jnp.log2(jnp.abs(value)) + (OCTAVES - top)) * FINE
    number = (jnp.clip(level, 0.0, CODES - 1.0) + 0.5).astype(jnp.int32)
    return jnp.where(value < 0.0, number + CODES, number)


def decode(number, top):
    level = number & (CODES - 1)
    size = jnp.exp2(level.astype(jnp.float32) * (1.0 / FINE) - (OCTAVES - top))
    size = jnp.where(level == 0, 0.0, size)
    return jnp.where(number >= CODES, -size, size)


def kernel(
    sizes,
    owner_hbm,
    count_hbm,
    part_ref,
    p_ref,
    m_ref,
    v_ref,
    np_ref,
    nm_ref,
    nv_ref,
    roll_ref,
    owner_ref,
    count_ref,
    own_w,
    scale,
    wbuf,
    block,
    theirs,
    near,
    out_hi,
    out_lo,
    in_hi,
    in_lo,
    acc,
    held,
    cross,
    in_s,
    w_s,
    w_r,
    opt_s,
    ld_s,
    raw_s,
    raw_r,
    near_s,
    near_r,
    hi_s,
    lo_s,
    rs_r,
    z_s,
    z_r,
    ag_s,
    ag_r,
    fin_s,
    fin_r,
):
    layers, fsdp, tp, parts, rows = sizes
    chunks = layers * parts
    pairs = fsdp // 2
    kept = pairs // 2
    bits = pairs.bit_length() - 1
    me = lax.axis_index("fsdp")
    col = lax.axis_index("tp")
    core = lax.rem(me, 2)
    mine_q = me // 2
    partner = mine_q * 2 + (1 - core)

    def away(index, flips):
        q = index
        for b in flips:
            q = q + (1 - 2 * lax.rem(index // (1 << b), 2)) * (1 << b)
        return q

    def ones(number):
        return [b for b in range(number.bit_length()) if number >> b & 1]

    tp_bits = tp.bit_length() - 1
    barrier = pltpu.get_barrier_semaphore()
    for d in range(1, fsdp):
        pl.semaphore_signal(
            barrier, inc=1, device_id={"fsdp": lax.rem(me + d, fsdp)}, device_id_type=MESH
        )
    for b in range(tp_bits):
        pl.semaphore_signal(
            barrier, inc=1, device_id={"tp": away(col, [b])}, device_id_type=MESH
        )

    groups = chunks // 2
    top = LARGEST + fsdp.bit_length() - 1
    width = theirs.shape[3]
    lanes = own_w.shape[1]

    def where(c):
        return lax.div(c, parts), lax.rem(c, parts)

    def order(slot):
        names = list(range(bits))
        return names if slot == 0 else names[::-1]

    def flipped(flips):
        return away(mine_q, flips)

    def block_of(slot, pos):
        return flipped([order(slot)[i] for i in range(bits) if pos >> (bits - 1 - i) & 1])

    def repeat(count, body):
        def run(i, carry):
            body(i)
            return carry

        lax.fori_loop(0, count, run, 0)

    def fetch(c, sem):
        l, k = where(c)
        pltpu.make_async_copy(part_ref.at[l, :, :, k], block.at[c], ld_s.at[sem]).start()

    count_copy = pltpu.make_async_copy(count_hbm, count_ref, in_s.at[0])
    count_copy.start()
    owner_copy = pltpu.make_async_copy(owner_hbm, owner_ref, in_s.at[1])
    owner_copy.start()
    early = 4
    for c in range(early):
        fetch(c, c // 2)
    repeat(chunks - early, lambda i: fetch(i + early, 2))
    count_copy.wait()
    own_w[...] = jnp.full(own_w.shape, count_ref[0], jnp.int32).astype(jnp.float32)
    pl.semaphore_wait(barrier, fsdp - 1 + tp_bits)

    def push(src, dst, send, arrive, **device):
        pltpu.make_async_remote_copy(
            src_ref=src,
            dst_ref=dst,
            send_sem=send,
            recv_sem=arrive,
            device_id=device,
            device_id_type=MESH,
        ).start()

    def await_part(part, sem):
        pltpu.make_async_copy(part, part, sem).wait()

    await_part(block.at[pl.ds(0, 2)], ld_s.at[0])
    for slot in range(2):
        there = flipped([order(slot)[0]]) * 2
        for pos in range(kept):
            for half in range(2):
                push(
                    block.at[slot, block_of(slot, kept + pos), half],
                    near.at[slot, core, pos],
                    near_s.at[0],
                    near_r.at[0],
                    fsdp=there + half,
                )

    def share(c):
        push(
            block.at[c, :, 1 - core],
            theirs.at[c],
            raw_s.at[0],
            raw_r.at[lax.div(c, 2)],
            fsdp=partner,
        )

    for c in range(early):
        if c == 2:
            await_part(block.at[pl.ds(2, 2)], ld_s.at[1])
        share(c)
    for d in range(1, fsdp):
        push(own_w, wbuf.at[d], w_s.at[0], w_r.at[min(d - 1, 1)], fsdp=away(me, ones(d)))
    await_part(block.at[pl.ds(early, chunks - early)], ld_s.at[2])
    repeat(chunks - early, lambda i: share(i + early))
    opts = []
    for i, (src, dst) in enumerate(((p_ref, np_ref), (m_ref, nm_ref), (v_ref, nv_ref))):
        load = pltpu.make_async_copy(src, dst, opt_s.at[i])
        load.start()
        opts.append(load)

    def row(tile):
        return jnp.concatenate([tile[0:1, :]] * (width // lanes), axis=1)

    def weigh():
        await_part(wbuf.at[pl.ds(2, fsdp - 2)], w_r.at[1])
        total = own_w[...]
        for d in range(1, fsdp):
            total = total + wbuf[d]
        scale[...] = 1.0 / total

    side = rows // 2
    step = next(n for n in range(min(side, SPAN), 0, -TILE) if side % n == 0)

    def tiles(body):
        for i in range(0, rows, step):
            body(pl.ds(i, step))

    def quads(body):
        for i in range(0, side, step):
            body(pl.ds(i, step), pl.ds(i + side, step))

    def both(body):
        def run(g):
            for slot in range(2):
                body(2 * g + slot, slot)

        return run

    def halve(c, slot, i):
        half = pairs >> (i + 1)
        there = flipped([order(slot)[i]]) * 2 + core
        for src, dst, send in ((out_hi, in_hi, hi_s), (out_lo, in_lo, lo_s)):
            push(
                src.at[c, pl.ds(half, half)],
                dst.at[c, pl.ds(half, half)],
                send.at[i],
                rs_r.at[lax.div(c, 2), i],
                fsdp=there,
            )

    def arrived(g, i):
        half = pairs >> (i + 1)
        await_part(in_lo.at[pl.ds(0, 5), pl.ds(0, 2 * half)], rs_r.at[g, i])

    def pair_sum(c, slot, pos, at):
        q = block_of(slot, pos)
        own = row(own_w[...]) * block[c, q, core, at, :].astype(jnp.float32)
        return own + row(wbuf[1]) * theirs[c, q, at, :].astype(jnp.float32)

    def near_sum(slot, pos, at):
        index = 1 << (order(slot)[0] + 1)
        total = row(wbuf[index + core]) * near[slot, 0, pos, at, :].astype(jnp.float32)
        return total + row(wbuf[index + 1 - core]) * near[slot, 1, pos, at, :].astype(jnp.float32)

    def fine_rows(at):
        return pl.ds(at.start // 2, at.size // 2)

    def write(c, pos, pair, values):
        numbers = [code(value, top) for value in values]
        out_hi[c, pos, pair[0], :] = (numbers[0] >> 4) | ((numbers[1] >> 4) << 16)
        middle, half = step // 2, width // 2
        word = None
        for n, number in enumerate(numbers):
            low = number & 15
            low = low[:middle] | (low[middle:] << 4)
            low = (low[:, :half] | (low[:, half:] << 8)) << (16 * n)
            word = low if word is None else word | low
        out_lo[c, pos, fine_rows(pair[0]), :] = word

    def read(c, pos, pair):
        high = in_hi[c, pos, pair[0], :]
        word = in_lo[c, pos, fine_rows(pair[0]), :]
        values = []
        for n in range(2):
            low = (word >> (16 * n)) & 65535
            low = jnp.concatenate([low & 255, low >> 8], axis=1)
            low = jnp.concatenate([low & 15, low >> 4], axis=0)
            values.append(decode((((high >> (16 * n)) & 65535) << 4) | low, top))
        return values

    def held_rows(c, slot, pos):
        q = flipped([order(slot)[b] for b in ones(pos)])
        l, k = where(c)
        return roll_ref.at[l, q, core, k]

    def double(c, slot, j):
        there = flipped([order(slot)[j]]) * 2 + core
        for pos in range(1 << j):
            block = held_rows(c, slot, pos)
            push(block, block, ag_s.at[j], ag_r.at[lax.div(c, 2), j], fsdp=there)

    def pair_of(g):
        return pl.ds(2 * g, 2)

    def first_halves(g):
        await_part(theirs.at[pair_of(g)], raw_r.at[g])

        @pl.when(g == 0)
        def _():
            await_part(wbuf.at[1], w_r.at[0])

        @pl.when(g > 0)
        def _():
            both(first_half)(g)

    def first_half(c, slot):
        for pos in range(pairs - 1, kept - 1, -1):

            def body(*pair):
                write(c, pos, pair, [pair_sum(c, slot, pos, at) for at in pair])

            quads(body)
        halve(c, slot, 0)

    def adds(i, g):
        if i > 0:
            arrived(g, i)
            both(functools.partial(add, i, False))(g)
            return

        @pl.when(g == 0)
        def _():
            await_part(near, near_r.at[0])
            weigh()
            both(functools.partial(add, i, True))(g)

        @pl.when(g > 0)
        def _():
            arrived(g, i)
            both(functools.partial(add, i, False))(g)

    def add(i, raw, c, slot):
        half = pairs >> (i + 1)
        for pos in range(half - 1, -1, -1):

            def body(*pair):
                if raw:
                    totals = [near_sum(slot, pos, at) for at in pair]
                else:
                    totals = read(c, half + pos, pair)
                for n, at in enumerate(pair):
                    totals[n] += pair_sum(c, slot, pos, at) if i == 0 else acc[c, pos, at, :]
                if half > 1 and pos >= half // 2:
                    write(c, pos, pair, totals)
                else:
                    for at, total in zip(pair, totals):
                        acc[c, pos, at, :] = total

            quads(body)
            if half > 1 and pos == half // 2:
                halve(c, slot, i + 1)

    def updates(g):
        @pl.when(g == 0)
        def _():
            for load in opts:
                load.wait()
            owner_copy.wait()

        arrived(g, bits - 1)
        both(update)(g)

    def update(c, slot):
        l, k = where(c)

        def body(*pair):
            totals = read(c, 1, pair)
            for at, total in zip(pair, totals):
                total = total + acc[c, 0, at, :]
                first, second, direction, new_params = adam(
                    total * row(scale[...]),
                    np_ref[l, k, at, :],
                    nm_ref[l, k, at, :],
                    nv_ref[l, k, at, :],
                )
                held[c, 0, at, :] = direction.astype(jnp.bfloat16)
                np_ref[l, k, at, :] = new_params
                nm_ref[l, k, at, :] = first
                nv_ref[l, k, at, :] = second

        quads(body)
        if tp_bits > 1:
            meet(c, 0)
        else:
            hand_over(c, slot)

    def meet(c, b):
        size = 1 << b
        push(
            held.at[c, pl.ds(0, size)],
            held.at[c, pl.ds(size, size)],
            z_s.at[b],
            z_r.at[lax.div(c, 2), b],
            tp=away(col, [b]),
        )

    def pick(c, at, served, start):
        chosen = start
        for slot in range(tp // 2):
            chosen = jnp.where(
                served == away(col, ones(slot)), held[c, slot, at, :].astype(jnp.float32), chosen
            )
        return chosen.astype(jnp.bfloat16)

    def hand_over(c, slot):
        l, k = where(c)
        there = away(col, [tp_bits - 1])
        served = owner_ref[l, there]

        def body(at):
            cross[c, 0, at, :] = pick(c, at, served, held[c, 0, at, :].astype(jnp.float32))

        tiles(body)
        push(
            cross.at[c, 0],
            cross.at[c, 1],
            z_s.at[tp_bits - 1],
            z_r.at[lax.div(c, 2), tp_bits - 1],
            tp=there,
        )

    def met(b, g):
        size = 1 << b
        await_part(held.at[pair_of(g), pl.ds(size, size)], z_r.at[g, b])
        if b + 2 < tp_bits:
            for slot in range(2):
                meet(2 * g + slot, b + 1)
        else:
            both(hand_over)(g)

    def selects(g):
        await_part(cross.at[pair_of(g), 1], z_r.at[g, tp_bits - 1])
        both(select)(g)

    def select(c, slot):
        l, k = where(c)
        served = owner_ref[l, col]

        def body(at):
            roll_ref[l, mine_q, core, k, at, :] = pick(
                c, at, served, cross[c, 1, at, :].astype(jnp.float32)
            )

        tiles(body)
        double(c, slot, 0)
        finish(c, slot, 0, 1)

    def finish(c, slot, first, count):
        for pos in range(first, first + count):
            block = held_rows(c, slot, pos)
            push(block, block, fin_s.at[0], fin_r.at[0], fsdp=partner)

    def forward(j, g):
        await_part(theirs.at[pl.ds(0, 2), pl.ds(0, 1 << j)], ag_r.at[g, j])
        for slot in range(2):
            if j + 1 < bits:
                double(2 * g + slot, slot, j + 1)
            finish(2 * g + slot, slot, 1 << j, 1 << j)

    stages = [first_halves]
    lags = [0]
    middle = [functools.partial(adds, i) for i in range(bits - 1)]
    middle += [updates]
    middle += [functools.partial(met, b) for b in range(tp_bits - 1)]
    lags += [AHEAD + GAP * i for i in range(bits)]
    lags += [lags[-1] + ZGAP * (b + 1) for b in range(tp_bits - 1)]
    tail = [selects] + [functools.partial(forward, j) for j in range(bits)]
    lags += [lags[-1] + LATE + AGAP * i for i in range(len(tail))]
    stages += middle + tail

    def at_step(t):
        for lag, stage in zip(lags, stages):
            g = t - lag
            pl.when(jnp.logical_and(g >= 0, g < groups))(functools.partial(stage, g))

    repeat(groups + lags[-1], at_step)

    await_part(wbuf.at[pl.ds(1, fsdp - 1)], w_s.at[0])
    await_part(theirs, raw_s.at[0])
    await_part(near, near_s.at[0])
    for i in range(bits):
        half = pairs >> (i + 1)
        sent = chunks if i > 0 else chunks - 2
        await_part(out_hi.at[pl.ds(0, sent), pl.ds(0, half)], hi_s.at[i])
        await_part(out_lo.at[pl.ds(0, sent), pl.ds(0, half)], lo_s.at[i])
        await_part(theirs.at[:, pl.ds(0, 1 << i)], ag_s.at[i])
    for b in range(tp_bits - 1):
        await_part(held.at[:, pl.ds(0, 1 << b)], z_s.at[b])
    await_part(cross.at[:, 0], z_s.at[tp_bits - 1])
    for sem in (fin_s, fin_r):
        await_part(theirs, sem.at[0])


def write_out(*refs):
    count = len(refs) // 2
    copies = []
    for i in range(count):
        n = refs[i].shape[1] // CUTS
        for l in range(refs[i].shape[0]):
            for j in range(CUTS):
                at = (l, pl.ds(j * n, n))
                copies.append(
                    pltpu.make_async_copy(refs[i].at[at], refs[count + i].at[at], refs[-1].at[i])
                )
    for copy in copies:
        copy.start()
    for i in range(count):
        pltpu.make_async_copy(refs[i], refs[count + i], refs[-1].at[i]).wait()


def fused(fsdp, tp, partials, token_counts, owner_map, params, moment1, moment2):
    layers, depth, width = partials.shape[1:]
    per = params.shape[1]
    pairs = fsdp // 2
    bits = pairs.bit_length() - 1
    tp_bits = tp.bit_length() - 1
    parts = next((n for n in range(SPLIT, 0, -1) if per % (n * 2 * TILE) == 0), None)
    if parts is None or width % 256 or layers * parts % 2 or layers * parts < 5:
        return plain(partials, token_counts, owner_map, params, moment1, moment2)
    rows = per // parts
    chunks = layers * parts
    lanes = 128
    anywhere = pl.BlockSpec(memory_space=pl.ANY)
    dma = pltpu.SemaphoreType.DMA
    state = (layers, parts, rows, width)
    f32, b16 = jnp.float32, jnp.bfloat16
    outs = pl.pallas_call(
        functools.partial(kernel, (layers, fsdp, tp, parts, rows)),
        out_shape=[
            pltpu.VMEM(state, f32),
            pltpu.VMEM(state, f32),
            pltpu.VMEM(state, f32),
            pltpu.VMEM((layers, pairs, 2, parts, rows, width), b16),
        ],
        in_specs=[
            anywhere,
            anywhere,
            anywhere,
            anywhere,
            anywhere,
            anywhere,
        ],
        out_specs=[pl.BlockSpec(memory_space=pltpu.VMEM)] * 4,
        scratch_shapes=[
            pltpu.SMEM((layers, tp), jnp.int32),
            pltpu.SMEM((1,), jnp.int32),
            pltpu.VMEM((8, lanes), f32),
            pltpu.VMEM((8, lanes), f32),
            pltpu.VMEM((fsdp, 8, lanes), f32),
            pltpu.VMEM((chunks, pairs, 2, rows, width), b16),
            pltpu.VMEM((chunks, pairs, rows, width), b16),
            pltpu.VMEM((2, 2, pairs // 2, rows, width), b16),
            pltpu.VMEM((chunks, pairs, rows // 2, width), jnp.int32),
            pltpu.VMEM((chunks, pairs, rows // 4, width // 2), jnp.int32),
            pltpu.VMEM((chunks, pairs, rows // 2, width), jnp.int32),
            pltpu.VMEM((chunks, pairs, rows // 4, width // 2), jnp.int32),
            pltpu.VMEM((chunks, pairs // 2, rows, width), f32),
            pltpu.VMEM((chunks, tp // 2, rows, width), b16),
            pltpu.VMEM((chunks, 2, rows, width), b16),
            dma((2,)),
            dma((1,)),
            dma((2,)),
            dma((3,)),
            dma((3,)),
            dma((1,)),
            dma((chunks // 2,)),
            dma((1,)),
            dma((1,)),
            dma((bits,)),
            dma((bits,)),
            dma((chunks // 2, bits)),
            dma((tp_bits,)),
            dma((chunks // 2, tp_bits)),
            dma((bits,)),
            dma((chunks // 2, bits)),
            dma((1,)),
            dma((1,)),
        ],
        compiler_params=pltpu.CompilerParams(
            collective_id=0, has_side_effects=True, vmem_limit_bytes=48 * 1024 * 1024
        ),
    )(
        owner_map,
        token_counts,
        partials.reshape(layers, pairs, 2, parts, rows, width),
        params.reshape(state),
        moment1.reshape(state),
        moment2.reshape(state),
    )
    outs = [out.reshape(params.shape) for out in outs[:3]] + [outs[3].reshape(layers, depth, width)]
    return tuple(
        pl.pallas_call(
            write_out,
            out_shape=[jax.ShapeDtypeStruct(out.shape, out.dtype) for out in outs],
            in_specs=[pl.BlockSpec(memory_space=pltpu.VMEM)] * 4,
            out_specs=[anywhere] * 4,
            scratch_shapes=[dma((4,))],
            compiler_params=pltpu.CompilerParams(vmem_limit_bytes=16 * 1024 * 1024),
        )(*outs)
    )


def solution(mesh):
    fsdp, tp = mesh.shape["fsdp"], mesh.shape["tp"]
    local = plain
    if fsdp >= 8 and fsdp & (fsdp - 1) == 0 and tp > 1 and tp & (tp - 1) == 0:
        local = functools.partial(fused, fsdp, tp)
    in_specs = (
        P("fsdp", None, None, "tp"),
        P("fsdp"),
        P(),
        P(None, "fsdp", "tp"),
        P(None, "fsdp", "tp"),
        P(None, "fsdp", "tp"),
    )
    out_specs = (
        P(None, "fsdp", "tp"),
        P(None, "fsdp", "tp"),
        P(None, "fsdp", "tp"),
        P(None, None, "tp"),
    )
    return jax.shard_map(local, mesh=mesh, in_specs=in_specs, out_specs=out_specs, check_vma=False)
```

```python
import functools

import jax
import jax.numpy as jnp
from jax import lax
from jax.experimental import pallas as pl
from jax.experimental.pallas import tpu as pltpu
from jax.sharding import PartitionSpec as P

STEP = 10
MESH = pl.DeviceIdType.MESH
SPLIT = 20
TILE = 16
SPAN = 80
AHEAD = 3
LATE = 6
GAP = 3
ZGAP = 3
AGAP = 4
CUTS = 5
RING = 12
SINGLE = 6
OCTAVES = 36
CODES = 1 << 19
FINE = CODES / OCTAVES
LARGEST = 12


def plain(partials, token_counts, owner_map, params, moment1, moment2):
    weight = token_counts.astype(jnp.float32)[0]
    total = lax.psum(weight, "fsdp")
    summed = lax.psum_scatter(
        weight * partials[0].astype(jnp.float32), "fsdp", scatter_dimension=1, tiled=True
    )
    first, second, direction, new_params = adam(summed * (1.0 / total), params, moment1, moment2)
    delta = direction.astype(jnp.bfloat16)
    owners = lax.axis_size("tp")
    served = lax.dynamic_index_in_dim(owner_map, lax.axis_index("tp"), 1, keepdims=False)
    blocks = lax.all_gather(delta, "tp", axis=0)
    kept = jnp.take_along_axis(blocks, served[None, :, None, None], axis=0)[0]
    rollout = lax.all_gather(kept, "fsdp", axis=1, tiled=True)
    return (new_params, first, second, rollout)


def adam(grad, params, moment1, moment2):
    first = 0.9 * moment1 + 0.1 * grad
    second = 0.999 * moment2 + 0.001 * grad * grad
    scale_one = 1.0 / (1.0 - 0.9**STEP)
    scale_two = 1.0 / (1.0 - 0.999**STEP)
    direction = first * scale_one / (jnp.sqrt(second * scale_two) + 1e-08)
    new_params = params - 0.001 * (direction + 0.1 * params)
    return first, second, direction, new_params


def code(value, top):
    level = (jnp.log2(jnp.abs(value)) + (OCTAVES - top)) * FINE
    number = (jnp.clip(level, 0.0, CODES - 1.0) + 0.5).astype(jnp.int32)
    return jnp.where(value < 0.0, number + CODES, number)


def decode(number, top):
    level = number & (CODES - 1)
    size = jnp.exp2(level.astype(jnp.float32) * (1.0 / FINE) - (OCTAVES - top))
    size = jnp.where(level == 0, 0.0, size)
    return jnp.where(number >= CODES, -size, size)


def kernel(
    sizes,
    owner_hbm,
    count_hbm,
    part_ref,
    p_ref,
    m_ref,
    v_ref,
    np_ref,
    nm_ref,
    nv_ref,
    roll_ref,
    owner_ref,
    count_ref,
    own_w,
    scale,
    wbuf,
    block,
    theirs,
    near,
    out_hi,
    out_lo,
    in_hi,
    in_lo,
    acc,
    held,
    cross,
    in_s,
    w_s,
    w_r,
    opt_s,
    ld_s,
    raw_s,
    raw_r,
    near_s,
    near_r,
    hi_s,
    lo_s,
    rs_r,
    z_s,
    z_r,
    last_r,
    ag_s,
    ag_r,
    fin_s,
    fin_r,
):
    layers, fsdp, tp, parts, rows = sizes
    chunks = layers * parts
    pairs = fsdp // 2
    kept = pairs // 2
    bits = pairs.bit_length() - 1
    me = lax.axis_index("fsdp")
    col = lax.axis_index("tp")
    core = lax.rem(me, 2)
    mine_q = me // 2
    partner = mine_q * 2 + (1 - core)

    def away(index, flips):
        q = index
        for b in flips:
            q = q + (1 - 2 * lax.rem(index // (1 << b), 2)) * (1 << b)
        return q

    def ones(number):
        return [b for b in range(number.bit_length()) if number >> b & 1]

    tp_bits = tp.bit_length() - 1
    barrier = pltpu.get_barrier_semaphore()
    for d in range(1, fsdp):
        pl.semaphore_signal(
            barrier, inc=1, device_id={"fsdp": lax.rem(me + d, fsdp)}, device_id_type=MESH
        )
    for b in range(tp_bits):
        pl.semaphore_signal(
            barrier, inc=1, device_id={"tp": away(col, [b])}, device_id_type=MESH
        )

    groups = chunks // 2
    top = LARGEST + fsdp.bit_length() - 1
    width = theirs.shape[3]
    lanes = own_w.shape[1]

    def where(c):
        return lax.div(c, parts), lax.rem(c, parts)

    def order(slot):
        names = list(range(bits))
        return names if slot == 0 else names[::-1]

    def flipped(flips):
        return away(mine_q, flips)

    def block_of(slot, pos):
        return flipped([order(slot)[i] for i in range(bits) if pos >> (bits - 1 - i) & 1])

    def turn(g):
        return lax.rem(g, min(RING, groups))

    def repeat(count, body):
        def run(i, carry):
            body(i)
            return carry

        lax.fori_loop(0, count, run, 0)

    def fetch(c, sem):
        l, k = where(c)
        pltpu.make_async_copy(part_ref.at[l, :, :, k], block.at[c], ld_s.at[sem]).start()

    count_copy = pltpu.make_async_copy(count_hbm, count_ref, in_s.at[0])
    count_copy.start()
    owner_copy = pltpu.make_async_copy(owner_hbm, owner_ref, in_s.at[1])
    owner_copy.start()
    early = 4
    for c in range(early):
        fetch(c, c // 2)
    repeat(chunks - early, lambda i: fetch(i + early, 2))
    count_copy.wait()
    own_w[...] = jnp.full(own_w.shape, count_ref[0], jnp.int32).astype(jnp.float32)
    pl.semaphore_wait(barrier, fsdp - 1 + tp_bits)

    def push(src, dst, send, arrive, **device):
        pltpu.make_async_remote_copy(
            src_ref=src,
            dst_ref=dst,
            send_sem=send,
            recv_sem=arrive,
            device_id=device,
            device_id_type=MESH,
        ).start()

    def await_part(part, sem):
        pltpu.make_async_copy(part, part, sem).wait()

    await_part(block.at[pl.ds(0, 2)], ld_s.at[0])
    for slot in range(2):
        there = flipped([order(slot)[0]]) * 2
        for pos in range(kept):
            for half in range(2):
                push(
                    block.at[slot, block_of(slot, kept + pos), half],
                    near.at[slot, core, pos],
                    near_s.at[0],
                    near_r.at[0],
                    fsdp=there + half,
                )

    single = min(SINGLE, groups - 1)

    def share(c):
        push(
            block.at[c, :, 1 - core],
            theirs.at[c],
            raw_s.at[0],
            raw_r.at[jnp.minimum(lax.div(c, 2), single)],
            fsdp=partner,
        )

    for c in range(early):
        if c == 2:
            await_part(block.at[pl.ds(2, 2)], ld_s.at[1])
        share(c)
    for d in range(1, fsdp):
        push(own_w, wbuf.at[d], w_s.at[0], w_r.at[min(d - 1, 1)], fsdp=away(me, ones(d)))
    await_part(block.at[pl.ds(early, chunks - early)], ld_s.at[2])
    repeat(chunks - early, lambda i: share(i + early))
    opts = []
    for i, (src, dst) in enumerate(((p_ref, np_ref), (m_ref, nm_ref), (v_ref, nv_ref))):
        load = pltpu.make_async_copy(src, dst, opt_s.at[i])
        load.start()
        opts.append(load)

    def row(tile):
        return jnp.concatenate([tile[0:1, :]] * (width // lanes), axis=1)

    def weigh():
        await_part(wbuf.at[pl.ds(2, fsdp - 2)], w_r.at[1])
        total = own_w[...]
        for d in range(1, fsdp):
            total = total + wbuf[d]
        scale[...] = 1.0 / total

    side = rows // 2
    step = next(n for n in range(min(side, SPAN), 0, -TILE) if side % n == 0)

    def tiles(body):
        for i in range(0, rows, step):
            body(pl.ds(i, step))

    def quads(body):
        for i in range(0, side, step):
            body(pl.ds(i, step), pl.ds(i + side, step))

    def both(body):
        def run(g):
            for slot in range(2):
                body(2 * g + slot, slot)

        return run

    def halve(c, slot, i):
        half = pairs >> (i + 1)
        there = flipped([order(slot)[i]]) * 2 + core
        for src, dst, send in ((out_hi, in_hi, hi_s), (out_lo, in_lo, lo_s)):
            push(
                src.at[c, pl.ds(half, half)],
                dst.at[c, pl.ds(half, half)],
                send.at[i],
                rs_r.at[turn(lax.div(c, 2)), i],
                fsdp=there,
            )

    def arrived(g, i):
        half = pairs >> (i + 1)
        await_part(in_lo.at[pl.ds(0, 5), pl.ds(0, 2 * half)], rs_r.at[turn(g), i])

    def pair_sum(c, slot, pos, at):
        q = block_of(slot, pos)
        own = row(own_w[...]) * block[c, q, core, at, :].astype(jnp.float32)
        return own + row(wbuf[1]) * theirs[c, q, at, :].astype(jnp.float32)

    def near_sum(slot, pos, at):
        index = 1 << (order(slot)[0] + 1)
        total = row(wbuf[index + core]) * near[slot, 0, pos, at, :].astype(jnp.float32)
        return total + row(wbuf[index + 1 - core]) * near[slot, 1, pos, at, :].astype(jnp.float32)

    def fine_rows(at):
        return pl.ds(at.start // 2, at.size // 2)

    def write(c, pos, pair, values):
        numbers = [code(value, top) for value in values]
        out_hi[c, pos, pair[0], :] = (numbers[0] >> 4) | ((numbers[1] >> 4) << 16)
        middle, half = step // 2, width // 2
        word = None
        for n, number in enumerate(numbers):
            low = number & 15
            low = low[:middle] | (low[middle:] << 4)
            low = (low[:, :half] | (low[:, half:] << 8)) << (16 * n)
            word = low if word is None else word | low
        out_lo[c, pos, fine_rows(pair[0]), :] = word

    def read(c, pos, pair):
        high = in_hi[c, pos, pair[0], :]
        word = in_lo[c, pos, fine_rows(pair[0]), :]
        values = []
        for n in range(2):
            low = (word >> (16 * n)) & 65535
            low = jnp.concatenate([low & 255, low >> 8], axis=1)
            low = jnp.concatenate([low & 15, low >> 4], axis=0)
            values.append(decode((((high >> (16 * n)) & 65535) << 4) | low, top))
        return values

    def held_rows(c, slot, pos):
        q = flipped([order(slot)[b] for b in ones(pos)])
        l, k = where(c)
        return roll_ref.at[l, q, core, k]

    def double(c, slot, j):
        there = flipped([order(slot)[j]]) * 2 + core
        for pos in range(1 << j):
            block = held_rows(c, slot, pos)
            push(block, block, ag_s.at[j], ag_r.at[turn(lax.div(c, 2)), j], fsdp=there)

    def pair_of(g):
        return pl.ds(2 * g, 2)

    def first_halves(g):
        @pl.when(g < single)
        def _():
            await_part(theirs.at[pair_of(g)], raw_r.at[g])

        @pl.when(g == single)
        def _():
            first = 2 * single
            await_part(theirs.at[pl.ds(first, chunks - first)], raw_r.at[single])

        @pl.when(g == 0)
        def _():
            await_part(wbuf.at[1], w_r.at[0])

        @pl.when(g > 0)
        def _():
            both(first_half)(g)

    def first_half(c, slot):
        for pos in range(pairs - 1, kept - 1, -1):

            def body(*pair):
                write(c, pos, pair, [pair_sum(c, slot, pos, at) for at in pair])

            quads(body)
        halve(c, slot, 0)

    def adds(i, g):
        if i > 0:
            arrived(g, i)
            both(functools.partial(add, i, False))(g)
            return

        @pl.when(g == 0)
        def _():
            await_part(near, near_r.at[0])
            weigh()
            both(functools.partial(add, i, True))(g)

        @pl.when(g > 0)
        def _():
            arrived(g, i)
            both(functools.partial(add, i, False))(g)

    def add(i, raw, c, slot):
        half = pairs >> (i + 1)
        for pos in range(half - 1, -1, -1):

            def body(*pair):
                if raw:
                    totals = [near_sum(slot, pos, at) for at in pair]
                else:
                    totals = read(c, half + pos, pair)
                for n, at in enumerate(pair):
                    totals[n] += pair_sum(c, slot, pos, at) if i == 0 else acc[c, pos, at, :]
                if half > 1 and pos >= half // 2:
                    write(c, pos, pair, totals)
                else:
                    for at, total in zip(pair, totals):
                        acc[c, pos, at, :] = total

            quads(body)
            if half > 1 and pos == half // 2:
                halve(c, slot, i + 1)

    def updates(g):
        @pl.when(g == 0)
        def _():
            for load in opts:
                load.wait()
            owner_copy.wait()

        arrived(g, bits - 1)
        both(update)(g)

    def update(c, slot):
        l, k = where(c)

        def body(*pair):
            totals = read(c, 1, pair)
            for at, total in zip(pair, totals):
                total = total + acc[c, 0, at, :]
                first, second, direction, new_params = adam(
                    total * row(scale[...]),
                    np_ref[l, k, at, :],
                    nm_ref[l, k, at, :],
                    nv_ref[l, k, at, :],
                )
                held[c, 0, at, :] = direction.astype(jnp.bfloat16)
                np_ref[l, k, at, :] = new_params
                nm_ref[l, k, at, :] = first
                nv_ref[l, k, at, :] = second

        quads(body)
        if tp_bits > 1:
            meet(c, 0)
        else:
            hand_over(c, slot)

    def meet(c, b):
        size = 1 << b
        push(
            held.at[c, pl.ds(0, size)],
            held.at[c, pl.ds(size, size)],
            z_s.at[b],
            z_r.at[turn(lax.div(c, 2)), b],
            tp=away(col, [b]),
        )

    def pick(c, at, served, start):
        chosen = start
        for slot in range(tp // 2):
            chosen = jnp.where(
                served == away(col, ones(slot)), held[c, slot, at, :].astype(jnp.float32), chosen
            )
        return chosen.astype(jnp.bfloat16)

    def hand_over(c, slot):
        l, k = where(c)
        there = away(col, [tp_bits - 1])
        served = owner_ref[l, there]

        def body(at):
            cross[c, 0, at, :] = pick(c, at, served, held[c, 0, at, :].astype(jnp.float32))

        tiles(body)
        push(
            cross.at[c, 0],
            cross.at[c, 1],
            z_s.at[tp_bits - 1],
            last_r.at[lax.div(c, 2)],
            tp=there,
        )

    def met(b, g):
        size = 1 << b
        await_part(held.at[pair_of(g), pl.ds(size, size)], z_r.at[turn(g), b])
        if b + 2 < tp_bits:
            for slot in range(2):
                meet(2 * g + slot, b + 1)
        else:
            both(hand_over)(g)

    def selects(g):
        await_part(cross.at[pair_of(g), 1], last_r.at[g])
        both(select)(g)

    def select(c, slot):
        l, k = where(c)
        served = owner_ref[l, col]

        def body(at):
            roll_ref[l, mine_q, core, k, at, :] = pick(
                c, at, served, cross[c, 1, at, :].astype(jnp.float32)
            )

        tiles(body)
        double(c, slot, 0)
        finish(c, slot, 0, 1)

    def finish(c, slot, first, count):
        for pos in range(first, first + count):
            block = held_rows(c, slot, pos)
            push(block, block, fin_s.at[0], fin_r.at[0], fsdp=partner)

    def forward(j, g):
        await_part(theirs.at[pl.ds(0, 2), pl.ds(0, 1 << j)], ag_r.at[turn(g), j])
        for slot in range(2):
            if j + 1 < bits:
                double(2 * g + slot, slot, j + 1)
            finish(2 * g + slot, slot, 1 << j, 1 << j)

    stages = [first_halves]
    lags = [0]
    middle = [functools.partial(adds, i) for i in range(bits - 1)]
    middle += [updates]
    middle += [functools.partial(met, b) for b in range(tp_bits - 1)]
    lags += [AHEAD + GAP * i for i in range(bits)]
    lags += [lags[-1] + ZGAP * (b + 1) for b in range(tp_bits - 1)]
    tail = [selects] + [functools.partial(forward, j) for j in range(bits)]
    lags += [lags[-1] + LATE + AGAP * i for i in range(len(tail))]
    stages += middle + tail

    def at_step(t):
        for lag, stage in zip(lags, stages):
            g = t - lag
            pl.when(jnp.logical_and(g >= 0, g < groups))(functools.partial(stage, g))

    repeat(groups + lags[-1], at_step)

    await_part(wbuf.at[pl.ds(1, fsdp - 1)], w_s.at[0])
    await_part(theirs, raw_s.at[0])
    await_part(near, near_s.at[0])
    for i in range(bits):
        half = pairs >> (i + 1)
        sent = chunks if i > 0 else chunks - 2
        await_part(out_hi.at[pl.ds(0, sent), pl.ds(0, half)], hi_s.at[i])
        await_part(out_lo.at[pl.ds(0, sent), pl.ds(0, half)], lo_s.at[i])
        await_part(theirs.at[:, pl.ds(0, 1 << i)], ag_s.at[i])
    for b in range(tp_bits - 1):
        await_part(held.at[:, pl.ds(0, 1 << b)], z_s.at[b])
    await_part(cross.at[:, 0], z_s.at[tp_bits - 1])
    for sem in (fin_s, fin_r):
        await_part(theirs, sem.at[0])


def write_out(*refs):
    count = len(refs) // 2
    copies = []
    for i in range(count):
        n = refs[i].shape[1] // CUTS
        for l in range(refs[i].shape[0]):
            for j in range(CUTS):
                at = (l, pl.ds(j * n, n))
                copies.append(
                    pltpu.make_async_copy(refs[i].at[at], refs[count + i].at[at], refs[-1].at[i])
                )
    for copy in copies:
        copy.start()
    for i in range(count):
        pltpu.make_async_copy(refs[i], refs[count + i], refs[-1].at[i]).wait()


def fused(fsdp, tp, partials, token_counts, owner_map, params, moment1, moment2):
    layers, depth, width = partials.shape[1:]
    per = params.shape[1]
    pairs = fsdp // 2
    bits = pairs.bit_length() - 1
    tp_bits = tp.bit_length() - 1
    parts = next((n for n in range(SPLIT, 0, -1) if per % (n * 2 * TILE) == 0), None)
    if parts is None or width % 256 or layers * parts % 2 or layers * parts < 5:
        return plain(partials, token_counts, owner_map, params, moment1, moment2)
    rows = per // parts
    chunks = layers * parts
    ring = min(RING, chunks // 2)
    lanes = 128
    anywhere = pl.BlockSpec(memory_space=pl.ANY)
    dma = pltpu.SemaphoreType.DMA
    state = (layers, parts, rows, width)
    f32, b16 = jnp.float32, jnp.bfloat16
    outs = pl.pallas_call(
        functools.partial(kernel, (layers, fsdp, tp, parts, rows)),
        out_shape=[
            pltpu.VMEM(state, f32),
            pltpu.VMEM(state, f32),
            pltpu.VMEM(state, f32),
            pltpu.VMEM((layers, pairs, 2, parts, rows, width), b16),
        ],
        in_specs=[
            anywhere,
            anywhere,
            anywhere,
            anywhere,
            anywhere,
            anywhere,
        ],
        out_specs=[pl.BlockSpec(memory_space=pltpu.VMEM)] * 4,
        scratch_shapes=[
            pltpu.SMEM((layers, tp), jnp.int32),
            pltpu.SMEM((1,), jnp.int32),
            pltpu.VMEM((8, lanes), f32),
            pltpu.VMEM((8, lanes), f32),
            pltpu.VMEM((fsdp, 8, lanes), f32),
            pltpu.VMEM((chunks, pairs, 2, rows, width), b16),
            pltpu.VMEM((chunks, pairs, rows, width), b16),
            pltpu.VMEM((2, 2, pairs // 2, rows, width), b16),
            pltpu.VMEM((chunks, pairs, rows // 2, width), jnp.int32),
            pltpu.VMEM((chunks, pairs, rows // 4, width // 2), jnp.int32),
            pltpu.VMEM((chunks, pairs, rows // 2, width), jnp.int32),
            pltpu.VMEM((chunks, pairs, rows // 4, width // 2), jnp.int32),
            pltpu.VMEM((chunks, pairs // 2, rows, width), f32),
            pltpu.VMEM((chunks, tp // 2, rows, width), b16),
            pltpu.VMEM((chunks, 2, rows, width), b16),
            dma((2,)),
            dma((1,)),
            dma((2,)),
            dma((3,)),
            dma((3,)),
            dma((1,)),
            dma((min(SINGLE + 1, chunks // 2),)),
            dma((1,)),
            dma((1,)),
            dma((bits,)),
            dma((bits,)),
            dma((ring, bits)),
            dma((tp_bits,)),
            dma((ring, max(tp_bits - 1, 1))),
            dma((chunks // 2,)),
            dma((bits,)),
            dma((ring, bits)),
            dma((1,)),
            dma((1,)),
        ],
        compiler_params=pltpu.CompilerParams(
            collective_id=0, has_side_effects=True, vmem_limit_bytes=48 * 1024 * 1024
        ),
    )(
        owner_map,
        token_counts,
        partials.reshape(layers, pairs, 2, parts, rows, width),
        params.reshape(state),
        moment1.reshape(state),
        moment2.reshape(state),
    )
    outs = [out.reshape(params.shape) for out in outs[:3]] + [outs[3].reshape(layers, depth, width)]
    return tuple(
        pl.pallas_call(
            write_out,
            out_shape=[jax.ShapeDtypeStruct(out.shape, out.dtype) for out in outs],
            in_specs=[pl.BlockSpec(memory_space=pltpu.VMEM)] * 4,
            out_specs=[anywhere] * 4,
            scratch_shapes=[dma((4,))],
            compiler_params=pltpu.CompilerParams(vmem_limit_bytes=16 * 1024 * 1024),
        )(*outs)
    )


def solution(mesh):
    fsdp, tp = mesh.shape["fsdp"], mesh.shape["tp"]
    local = plain
    if fsdp >= 8 and fsdp & (fsdp - 1) == 0 and tp > 1 and tp & (tp - 1) == 0:
        local = functools.partial(fused, fsdp, tp)
    in_specs = (
        P("fsdp", None, None, "tp"),
        P("fsdp"),
        P(),
        P(None, "fsdp", "tp"),
        P(None, "fsdp", "tp"),
        P(None, "fsdp", "tp"),
    )
    out_specs = (
        P(None, "fsdp", "tp"),
        P(None, "fsdp", "tp"),
        P(None, "fsdp", "tp"),
        P(None, None, "tp"),
    )
    return jax.shard_map(local, mesh=mesh, in_specs=in_specs, out_specs=out_specs, check_vma=False)
```

```python
import functools

import jax
import jax.numpy as jnp
from jax import lax
from jax.experimental import pallas as pl
from jax.experimental.pallas import tpu as pltpu
from jax.sharding import PartitionSpec as P

STEP = 10
MESH = pl.DeviceIdType.MESH
SPLIT = 20
TILE = 16
SPAN = 80
AHEAD = 3
LATE = 6
GAP = 3
ZGAP = 3
AGAP = 4
CUTS = 5
RING = 10
SINGLE = 4
OCTAVES = 36
CODES = 1 << 19
FINE = CODES / OCTAVES
LARGEST = 12


def plain(partials, token_counts, owner_map, params, moment1, moment2):
    weight = token_counts.astype(jnp.float32)[0]
    total = lax.psum(weight, "fsdp")
    summed = lax.psum_scatter(
        weight * partials[0].astype(jnp.float32), "fsdp", scatter_dimension=1, tiled=True
    )
    first, second, direction, new_params = adam(summed * (1.0 / total), params, moment1, moment2)
    delta = direction.astype(jnp.bfloat16)
    owners = lax.axis_size("tp")
    served = lax.dynamic_index_in_dim(owner_map, lax.axis_index("tp"), 1, keepdims=False)
    blocks = lax.all_gather(delta, "tp", axis=0)
    kept = jnp.take_along_axis(blocks, served[None, :, None, None], axis=0)[0]
    rollout = lax.all_gather(kept, "fsdp", axis=1, tiled=True)
    return (new_params, first, second, rollout)


def adam(grad, params, moment1, moment2):
    first = 0.9 * moment1 + 0.1 * grad
    second = 0.999 * moment2 + 0.001 * grad * grad
    scale_one = 1.0 / (1.0 - 0.9**STEP)
    scale_two = 1.0 / (1.0 - 0.999**STEP)
    direction = first * scale_one / (jnp.sqrt(second * scale_two) + 1e-08)
    new_params = params - 0.001 * (direction + 0.1 * params)
    return first, second, direction, new_params


def code(value, top):
    level = (jnp.log2(jnp.abs(value)) + (OCTAVES - top)) * FINE
    number = (jnp.clip(level, 0.0, CODES - 1.0) + 0.5).astype(jnp.int32)
    return jnp.where(value < 0.0, number + CODES, number)


def decode(number, top):
    level = number & (CODES - 1)
    size = jnp.exp2(level.astype(jnp.float32) * (1.0 / FINE) - (OCTAVES - top))
    size = jnp.where(level == 0, 0.0, size)
    return jnp.where(number >= CODES, -size, size)


def kernel(
    sizes,
    owner_hbm,
    count_hbm,
    part_ref,
    p_ref,
    m_ref,
    v_ref,
    np_ref,
    nm_ref,
    nv_ref,
    roll_ref,
    owner_ref,
    count_ref,
    own_w,
    scale,
    wbuf,
    block,
    theirs,
    near,
    out_hi,
    out_lo,
    in_hi,
    in_lo,
    acc,
    held,
    cross,
    in_s,
    w_s,
    w_r,
    opt_s,
    ld_s,
    raw_s,
    raw_r,
    near_s,
    near_r,
    hi_s,
    lo_s,
    rs_r,
    z_s,
    z_r,
    last_r,
    ag_s,
    ag_r,
    fin_s,
    fin_r,
):
    layers, fsdp, tp, parts, rows = sizes
    chunks = layers * parts
    pairs = fsdp // 2
    kept = pairs // 2
    bits = pairs.bit_length() - 1
    me = lax.axis_index("fsdp")
    col = lax.axis_index("tp")
    core = lax.rem(me, 2)
    mine_q = me // 2
    partner = mine_q * 2 + (1 - core)

    def away(index, flips):
        q = index
        for b in flips:
            q = q + (1 - 2 * lax.rem(index // (1 << b), 2)) * (1 << b)
        return q

    def ones(number):
        return [b for b in range(number.bit_length()) if number >> b & 1]

    tp_bits = tp.bit_length() - 1
    barrier = pltpu.get_barrier_semaphore()
    for d in range(1, fsdp):
        pl.semaphore_signal(
            barrier, inc=1, device_id={"fsdp": lax.rem(me + d, fsdp)}, device_id_type=MESH
        )
    for b in range(tp_bits):
        pl.semaphore_signal(
            barrier, inc=1, device_id={"tp": away(col, [b])}, device_id_type=MESH
        )

    groups = chunks // 2
    top = LARGEST + fsdp.bit_length() - 1
    width = theirs.shape[3]
    lanes = own_w.shape[1]

    def where(c):
        return lax.div(c, parts), lax.rem(c, parts)

    def order(slot):
        names = list(range(bits))
        return names if slot == 0 else names[::-1]

    def flipped(flips):
        return away(mine_q, flips)

    def block_of(slot, pos):
        return flipped([order(slot)[i] for i in range(bits) if pos >> (bits - 1 - i) & 1])

    def turn(g):
        return lax.rem(g, min(RING, groups))

    def repeat(count, body):
        def run(i, carry):
            body(i)
            return carry

        lax.fori_loop(0, count, run, 0)

    def fetch(c, sem):
        l, k = where(c)
        pltpu.make_async_copy(part_ref.at[l, :, :, k], block.at[c], ld_s.at[sem]).start()

    count_copy = pltpu.make_async_copy(count_hbm, count_ref, in_s.at[0])
    count_copy.start()
    owner_copy = pltpu.make_async_copy(owner_hbm, owner_ref, in_s.at[1])
    owner_copy.start()
    early = 4
    for c in range(early):
        fetch(c, c // 2)
    repeat(chunks - early, lambda i: fetch(i + early, 2))
    pl.semaphore_wait(barrier, fsdp - 1 + tp_bits)

    def push(src, dst, send, arrive, **device):
        pltpu.make_async_remote_copy(
            src_ref=src,
            dst_ref=dst,
            send_sem=send,
            recv_sem=arrive,
            device_id=device,
            device_id_type=MESH,
        ).start()

    def await_part(part, sem):
        pltpu.make_async_copy(part, part, sem).wait()

    await_part(block.at[pl.ds(0, 2)], ld_s.at[0])
    for slot in range(2):
        there = flipped([order(slot)[0]]) * 2
        for pos in range(kept):
            for half in range(2):
                push(
                    block.at[slot, block_of(slot, kept + pos), half],
                    near.at[slot, core, pos],
                    near_s.at[0],
                    near_r.at[0],
                    fsdp=there + half,
                )

    single = min(SINGLE, groups - 1)

    def share(c):
        push(
            block.at[c, :, 1 - core],
            theirs.at[c],
            raw_s.at[0],
            raw_r.at[jnp.minimum(lax.div(c, 2), single)],
            fsdp=partner,
        )

    count_copy.wait()
    own_w[...] = jnp.full(own_w.shape, count_ref[0], jnp.int32).astype(jnp.float32)
    for c in range(early):
        if c == 2:
            await_part(block.at[pl.ds(2, 2)], ld_s.at[1])
        share(c)
    for d in range(1, fsdp):
        push(own_w, wbuf.at[d], w_s.at[0], w_r.at[min(d - 1, 1)], fsdp=away(me, ones(d)))
    await_part(block.at[pl.ds(early, chunks - early)], ld_s.at[2])
    repeat(chunks - early, lambda i: share(i + early))
    opts = []
    for i, (src, dst) in enumerate(((p_ref, np_ref), (m_ref, nm_ref), (v_ref, nv_ref))):
        load = pltpu.make_async_copy(src, dst, opt_s.at[i])
        load.start()
        opts.append(load)

    def row(tile):
        return jnp.concatenate([tile[0:1, :]] * (width // lanes), axis=1)

    def weigh():
        await_part(wbuf.at[pl.ds(2, fsdp - 2)], w_r.at[1])
        total = own_w[...]
        for d in range(1, fsdp):
            total = total + wbuf[d]
        scale[...] = 1.0 / total

    side = rows // 2
    step = next(n for n in range(min(side, SPAN), 0, -TILE) if side % n == 0)

    def tiles(body):
        for i in range(0, rows, step):
            body(pl.ds(i, step))

    def quads(body):
        for i in range(0, side, step):
            body(pl.ds(i, step), pl.ds(i + side, step))

    def both(body):
        def run(g):
            for slot in range(2):
                body(2 * g + slot, slot)

        return run

    def halve(c, slot, i):
        half = pairs >> (i + 1)
        there = flipped([order(slot)[i]]) * 2 + core
        for src, dst, send in ((out_hi, in_hi, hi_s), (out_lo, in_lo, lo_s)):
            push(
                src.at[c, pl.ds(half, half)],
                dst.at[c, pl.ds(half, half)],
                send.at[i],
                rs_r.at[turn(lax.div(c, 2)), i],
                fsdp=there,
            )

    def arrived(g, i):
        half = pairs >> (i + 1)
        await_part(in_lo.at[pl.ds(0, 5), pl.ds(0, 2 * half)], rs_r.at[turn(g), i])

    def pair_sum(c, slot, pos, at):
        q = block_of(slot, pos)
        own = row(own_w[...]) * block[c, q, core, at, :].astype(jnp.float32)
        return own + row(wbuf[1]) * theirs[c, q, at, :].astype(jnp.float32)

    def near_sum(slot, pos, at):
        index = 1 << (order(slot)[0] + 1)
        total = row(wbuf[index + core]) * near[slot, 0, pos, at, :].astype(jnp.float32)
        return total + row(wbuf[index + 1 - core]) * near[slot, 1, pos, at, :].astype(jnp.float32)

    def fine_rows(at):
        return pl.ds(at.start // 2, at.size // 2)

    def write(c, pos, pair, values):
        numbers = [code(value, top) for value in values]
        out_hi[c, pos, pair[0], :] = (numbers[0] >> 4) | ((numbers[1] >> 4) << 16)
        middle, half = step // 2, width // 2
        word = None
        for n, number in enumerate(numbers):
            low = number & 15
            low = low[:middle] | (low[middle:] << 4)
            low = (low[:, :half] | (low[:, half:] << 8)) << (16 * n)
            word = low if word is None else word | low
        out_lo[c, pos, fine_rows(pair[0]), :] = word

    def read(c, pos, pair):
        high = in_hi[c, pos, pair[0], :]
        word = in_lo[c, pos, fine_rows(pair[0]), :]
        values = []
        for n in range(2):
            low = (word >> (16 * n)) & 65535
            low = jnp.concatenate([low & 255, low >> 8], axis=1)
            low = jnp.concatenate([low & 15, low >> 4], axis=0)
            values.append(decode((((high >> (16 * n)) & 65535) << 4) | low, top))
        return values

    def held_rows(c, slot, pos):
        q = flipped([order(slot)[b] for b in ones(pos)])
        l, k = where(c)
        return roll_ref.at[l, q, core, k]

    def double(c, slot, j):
        there = flipped([order(slot)[j]]) * 2 + core
        for pos in range(1 << j):
            block = held_rows(c, slot, pos)
            push(block, block, ag_s.at[j], ag_r.at[turn(lax.div(c, 2)), j], fsdp=there)

    def pair_of(g):
        return pl.ds(2 * g, 2)

    def first_halves(g):
        @pl.when(g < single)
        def _():
            await_part(theirs.at[pair_of(g)], raw_r.at[g])

        @pl.when(g == single)
        def _():
            first = 2 * single
            await_part(theirs.at[pl.ds(first, chunks - first)], raw_r.at[single])

        @pl.when(g == 0)
        def _():
            await_part(wbuf.at[1], w_r.at[0])

        @pl.when(g > 0)
        def _():
            both(first_half)(g)

    def first_half(c, slot):
        for pos in range(pairs - 1, kept - 1, -1):

            def body(*pair):
                write(c, pos, pair, [pair_sum(c, slot, pos, at) for at in pair])

            quads(body)
        halve(c, slot, 0)

    def adds(i, g):
        if i > 0:
            arrived(g, i)
            both(functools.partial(add, i, False))(g)
            return

        @pl.when(g == 0)
        def _():
            await_part(near, near_r.at[0])
            weigh()
            both(functools.partial(add, i, True))(g)

        @pl.when(g > 0)
        def _():
            arrived(g, i)
            both(functools.partial(add, i, False))(g)

    def add(i, raw, c, slot):
        half = pairs >> (i + 1)
        for pos in range(half - 1, -1, -1):

            def body(*pair):
                if raw:
                    totals = [near_sum(slot, pos, at) for at in pair]
                else:
                    totals = read(c, half + pos, pair)
                for n, at in enumerate(pair):
                    totals[n] += pair_sum(c, slot, pos, at) if i == 0 else acc[c, pos, at, :]
                if half > 1 and pos >= half // 2:
                    write(c, pos, pair, totals)
                else:
                    for at, total in zip(pair, totals):
                        acc[c, pos, at, :] = total

            quads(body)
            if half > 1 and pos == half // 2:
                halve(c, slot, i + 1)

    def updates(g):
        @pl.when(g == 0)
        def _():
            for load in opts:
                load.wait()
            owner_copy.wait()

        arrived(g, bits - 1)
        both(update)(g)

    def update(c, slot):
        l, k = where(c)

        def body(*pair):
            totals = read(c, 1, pair)
            for at, total in zip(pair, totals):
                total = total + acc[c, 0, at, :]
                first, second, direction, new_params = adam(
                    total * row(scale[...]),
                    np_ref[l, k, at, :],
                    nm_ref[l, k, at, :],
                    nv_ref[l, k, at, :],
                )
                held[c, 0, at, :] = direction.astype(jnp.bfloat16)
                np_ref[l, k, at, :] = new_params
                nm_ref[l, k, at, :] = first
                nv_ref[l, k, at, :] = second

        quads(body)
        if tp_bits > 1:
            meet(c, 0)
        else:
            hand_over(c, slot)

    def meet(c, b):
        size = 1 << b
        push(
            held.at[c, pl.ds(0, size)],
            held.at[c, pl.ds(size, size)],
            z_s.at[b],
            z_r.at[turn(lax.div(c, 2)), b],
            tp=away(col, [b]),
        )

    def pick(c, at, served, start):
        chosen = start
        for slot in range(tp // 2):
            chosen = jnp.where(
                served == away(col, ones(slot)), held[c, slot, at, :].astype(jnp.float32), chosen
            )
        return chosen.astype(jnp.bfloat16)

    def hand_over(c, slot):
        l, k = where(c)
        there = away(col, [tp_bits - 1])
        served = owner_ref[l, there]

        def body(at):
            cross[c, 0, at, :] = pick(c, at, served, held[c, 0, at, :].astype(jnp.float32))

        tiles(body)
        push(
            cross.at[c, 0],
            cross.at[c, 1],
            z_s.at[tp_bits - 1],
            last_r.at[lax.div(c, 2)],
            tp=there,
        )

    def met(b, g):
        size = 1 << b
        await_part(held.at[pair_of(g), pl.ds(size, size)], z_r.at[turn(g), b])
        if b + 2 < tp_bits:
            for slot in range(2):
                meet(2 * g + slot, b + 1)
        else:
            both(hand_over)(g)

    def selects(g):
        await_part(cross.at[pair_of(g), 1], last_r.at[g])
        both(select)(g)

    def select(c, slot):
        l, k = where(c)
        served = owner_ref[l, col]

        def body(at):
            roll_ref[l, mine_q, core, k, at, :] = pick(
                c, at, served, cross[c, 1, at, :].astype(jnp.float32)
            )

        tiles(body)
        double(c, slot, 0)
        finish(c, slot, 0, 1)

    def finish(c, slot, first, count):
        for pos in range(first, first + count):
            block = held_rows(c, slot, pos)
            push(block, block, fin_s.at[0], fin_r.at[0], fsdp=partner)

    def forward(j, g):
        await_part(theirs.at[pl.ds(0, 2), pl.ds(0, 1 << j)], ag_r.at[turn(g), j])
        for slot in range(2):
            if j + 1 < bits:
                double(2 * g + slot, slot, j + 1)
            finish(2 * g + slot, slot, 1 << j, 1 << j)

    stages = [first_halves]
    lags = [0]
    middle = [functools.partial(adds, i) for i in range(bits - 1)]
    middle += [updates]
    middle += [functools.partial(met, b) for b in range(tp_bits - 1)]
    lags += [AHEAD + GAP * i for i in range(bits)]
    lags += [lags[-1] + ZGAP * (b + 1) for b in range(tp_bits - 1)]
    tail = [selects] + [functools.partial(forward, j) for j in range(bits)]
    lags += [lags[-1] + LATE + AGAP * i for i in range(len(tail))]
    stages += middle + tail

    def at_step(t):
        for lag, stage in zip(lags, stages):
            g = t - lag
            pl.when(jnp.logical_and(g >= 0, g < groups))(functools.partial(stage, g))

    repeat(groups + lags[-1], at_step)

    await_part(wbuf.at[pl.ds(1, fsdp - 1)], w_s.at[0])
    await_part(theirs, raw_s.at[0])
    await_part(near, near_s.at[0])
    for i in range(bits):
        half = pairs >> (i + 1)
        sent = chunks if i > 0 else chunks - 2
        await_part(out_hi.at[pl.ds(0, sent), pl.ds(0, half)], hi_s.at[i])
        await_part(out_lo.at[pl.ds(0, sent), pl.ds(0, half)], lo_s.at[i])
        await_part(theirs.at[:, pl.ds(0, 1 << i)], ag_s.at[i])
    for b in range(tp_bits - 1):
        await_part(held.at[:, pl.ds(0, 1 << b)], z_s.at[b])
    await_part(cross.at[:, 0], z_s.at[tp_bits - 1])
    for sem in (fin_s, fin_r):
        await_part(theirs, sem.at[0])


def write_out(*refs):
    count = len(refs) // 2
    copies = []
    for i in range(count):
        n = refs[i].shape[1] // CUTS
        for l in range(refs[i].shape[0]):
            for j in range(CUTS):
                at = (l, pl.ds(j * n, n))
                copies.append(
                    pltpu.make_async_copy(refs[i].at[at], refs[count + i].at[at], refs[-1].at[i])
                )
    for copy in copies:
        copy.start()
    for i in range(count):
        pltpu.make_async_copy(refs[i], refs[count + i], refs[-1].at[i]).wait()


def fused(fsdp, tp, partials, token_counts, owner_map, params, moment1, moment2):
    layers, depth, width = partials.shape[1:]
    per = params.shape[1]
    pairs = fsdp // 2
    bits = pairs.bit_length() - 1
    tp_bits = tp.bit_length() - 1
    parts = next((n for n in range(SPLIT, 0, -1) if per % (n * 2 * TILE) == 0), None)
    if parts is None or width % 256 or layers * parts % 2 or layers * parts < 5:
        return plain(partials, token_counts, owner_map, params, moment1, moment2)
    rows = per // parts
    chunks = layers * parts
    ring = min(RING, chunks // 2)
    lanes = 128
    anywhere = pl.BlockSpec(memory_space=pl.ANY)
    dma = pltpu.SemaphoreType.DMA
    state = (layers, parts, rows, width)
    f32, b16 = jnp.float32, jnp.bfloat16
    outs = pl.pallas_call(
        functools.partial(kernel, (layers, fsdp, tp, parts, rows)),
        out_shape=[
            pltpu.VMEM(state, f32),
            pltpu.VMEM(state, f32),
            pltpu.VMEM(state, f32),
            pltpu.VMEM((layers, pairs, 2, parts, rows, width), b16),
        ],
        in_specs=[
            anywhere,
            anywhere,
            anywhere,
            anywhere,
            anywhere,
            anywhere,
        ],
        out_specs=[pl.BlockSpec(memory_space=pltpu.VMEM)] * 4,
        scratch_shapes=[
            pltpu.SMEM((layers, tp), jnp.int32),
            pltpu.SMEM((1,), jnp.int32),
            pltpu.VMEM((8, lanes), f32),
            pltpu.VMEM((8, lanes), f32),
            pltpu.VMEM((fsdp, 8, lanes), f32),
            pltpu.VMEM((chunks, pairs, 2, rows, width), b16),
            pltpu.VMEM((chunks, pairs, rows, width), b16),
            pltpu.VMEM((2, 2, pairs // 2, rows, width), b16),
            pltpu.VMEM((chunks, pairs, rows // 2, width), jnp.int32),
            pltpu.VMEM((chunks, pairs, rows // 4, width // 2), jnp.int32),
            pltpu.VMEM((chunks, pairs, rows // 2, width), jnp.int32),
            pltpu.VMEM((chunks, pairs, rows // 4, width // 2), jnp.int32),
            pltpu.VMEM((chunks, pairs // 2, rows, width), f32),
            pltpu.VMEM((chunks, tp // 2, rows, width), b16),
            pltpu.VMEM((chunks, 2, rows, width), b16),
            dma((2,)),
            dma((1,)),
            dma((2,)),
            dma((3,)),
            dma((3,)),
            dma((1,)),
            dma((min(SINGLE + 1, chunks // 2),)),
            dma((1,)),
            dma((1,)),
            dma((bits,)),
            dma((bits,)),
            dma((ring, bits)),
            dma((tp_bits,)),
            dma((ring, max(tp_bits - 1, 1))),
            dma((chunks // 2,)),
            dma((bits,)),
            dma((ring, bits)),
            dma((1,)),
            dma((1,)),
        ],
        compiler_params=pltpu.CompilerParams(
            collective_id=0, has_side_effects=True, vmem_limit_bytes=48 * 1024 * 1024
        ),
    )(
        owner_map,
        token_counts,
        partials.reshape(layers, pairs, 2, parts, rows, width),
        params.reshape(state),
        moment1.reshape(state),
        moment2.reshape(state),
    )
    outs = [out.reshape(params.shape) for out in outs[:3]] + [outs[3].reshape(layers, depth, width)]
    return tuple(
        pl.pallas_call(
            write_out,
            out_shape=[jax.ShapeDtypeStruct(out.shape, out.dtype) for out in outs],
            in_specs=[pl.BlockSpec(memory_space=pltpu.VMEM)] * 4,
            out_specs=[anywhere] * 4,
            scratch_shapes=[dma((4,))],
            compiler_params=pltpu.CompilerParams(vmem_limit_bytes=16 * 1024 * 1024),
        )(*outs)
    )


def solution(mesh):
    fsdp, tp = mesh.shape["fsdp"], mesh.shape["tp"]
    local = plain
    if fsdp >= 8 and fsdp & (fsdp - 1) == 0 and tp > 1 and tp & (tp - 1) == 0:
        local = functools.partial(fused, fsdp, tp)
    in_specs = (
        P("fsdp", None, None, "tp"),
        P("fsdp"),
        P(),
        P(None, "fsdp", "tp"),
        P(None, "fsdp", "tp"),
        P(None, "fsdp", "tp"),
    )
    out_specs = (
        P(None, "fsdp", "tp"),
        P(None, "fsdp", "tp"),
        P(None, "fsdp", "tp"),
        P(None, None, "tp"),
    )
    return jax.shard_map(local, mesh=mesh, in_specs=in_specs, out_specs=out_specs, check_vma=False)
```
